32 devices in a mesh: dp: 2 (over x), tp: 4 (over z), sp: 4 (over y, core).
Axes of the slice: x: 2, y: 2, z: 4, core: 2. Of those that a mesh axis runs over, the one named last changes fastest.
Arguments:
- x: bfloat16 [12, 64, 128, 1024], P('dp', 'sp'), parts along dimension 0
- w_qkv: bfloat16 [1024, 3, 1024], P(None, None, 'tp')
- q_bias: bfloat16 [1024], P('tp')
- v_bias: bfloat16 [1024], P('tp')
- logit_scale: float32 [32], P('tp')
- cpb_w1: float32 [2, 512], replicated
- cpb_b1: float32 [512], replicated
- cpb_w2: float32 [512, 32], replicated
- w_proj: bfloat16 [1024, 1024], P('tp')
- b_proj: bfloat16 [1024], replicated
- ln1_gain: float32 [1024], replicated
- ln1_bias: float32 [1024], replicated
- w_fc1: bfloat16 [1024, 4096], P(None, 'tp')
- b_fc1: bfloat16 [4096], P('tp')
- w_fc2: bfloat16 [4096, 1024], P('tp')
- b_fc2: bfloat16 [1024], replicated
- ln2_gain: float32 [1024], replicated
- ln2_bias: float32 [1024], replicated
Outputs:
- output: bfloat16 [12, 64, 128, 1024], P('dp', 'sp'), parts along dimension 0
There are 2 independent parts. The reference program is written for one: setup_inputs(seed, part) draws one part's arguments, and reference() takes and returns one part's arrays. A program takes and returns all parts, laid end to end along the dimension named above; an argument that names none is the same for every part.
All inputs are finite; a program needn't handle non-finite values.
Results may differ from the reference program's by a relative error of at most 0.0142195.
Values are sent between devices in bfloat16 or wider.
A program may use at most 1 GiB of HBM per device.

```python
import math
import jax
import jax.numpy as jnp
from jax import lax

BATCH = 6
HEIGHT = 64
WIDTH = 128
CHANNELS = 1024
N_HEADS = 32
WINDOW = 16
CPB_HIDDEN = 512
SHIFT = WINDOW // 2
MLP_WIDTH = 4 * CHANNELS
HEAD_DIM = CHANNELS // N_HEADS
LN_EPS = 1e-5
NORM_EPS = 1e-12


def draw_normal(wkeys, key_num, arr_shape, spread):
    return spread * jax.random.normal(wkeys[key_num], arr_shape, jnp.float32)


def setup_inputs(seed: int = 0, part: int = 0) -> dict:
    wkeys = jax.random.split(jax.random.key(seed), 17)
    x_key = jax.random.fold_in(jax.random.key(seed + 1), part)
    noise_key, profile_key = jax.random.split(x_key)
    noise = jax.random.normal(noise_key, (BATCH, HEIGHT, WIDTH, CHANNELS), jnp.float32)
    profile = jax.random.normal(profile_key, (BATCH, HEIGHT, 1, CHANNELS), jnp.float32)
    return {
        'x': (noise + 0.7 * profile).astype(jnp.bfloat16),
        'w_qkv': draw_normal(wkeys, 0, (CHANNELS, 3, CHANNELS), CHANNELS ** -0.5).astype(jnp.bfloat16),
        'q_bias': draw_normal(wkeys, 1, (CHANNELS,), 0.3).astype(jnp.bfloat16),
        'v_bias': draw_normal(wkeys, 2, (CHANNELS,), 0.2).astype(jnp.bfloat16),
        'logit_scale': jax.random.uniform(wkeys[3], (N_HEADS,), jnp.float32, minval=math.log(4.0), maxval=math.log(120.0)),
        'cpb_w1': draw_normal(wkeys, 4, (2, CPB_HIDDEN), 1.0),
        'cpb_b1': draw_normal(wkeys, 5, (CPB_HIDDEN,), 0.5),
        'cpb_w2': draw_normal(wkeys, 6, (CPB_HIDDEN, N_HEADS), 1.5 * CPB_HIDDEN ** -0.5),
        'w_proj': draw_normal(wkeys, 7, (CHANNELS, CHANNELS), CHANNELS ** -0.5).astype(jnp.bfloat16),
        'b_proj': draw_normal(wkeys, 8, (CHANNELS,), 0.2).astype(jnp.bfloat16),
        'ln1_gain': 1.0 + draw_normal(wkeys, 9, (CHANNELS,), 0.3),
        'ln1_bias': draw_normal(wkeys, 10, (CHANNELS,), 0.3),
        'w_fc1': draw_normal(wkeys, 11, (CHANNELS, MLP_WIDTH), CHANNELS ** -0.5).astype(jnp.bfloat16),
        'b_fc1': draw_normal(wkeys, 12, (MLP_WIDTH,), 0.5).astype(jnp.bfloat16),
        'w_fc2': draw_normal(wkeys, 13, (MLP_WIDTH, CHANNELS), MLP_WIDTH ** -0.5).astype(jnp.bfloat16),
        'b_fc2': draw_normal(wkeys, 14, (CHANNELS,), 0.2).astype(jnp.bfloat16),
        'ln2_gain': 1.0 + draw_normal(wkeys, 15, (CHANNELS,), 0.3),
        'ln2_bias': draw_normal(wkeys, 16, (CHANNELS,), 0.3),
    }


def layer_norm(values, ln_gain, ln_bias):
    row_mean = jnp.mean(values, axis=-1, keepdims=True)
    centred = values - row_mean
    row_var = jnp.mean(centred * centred, axis=-1, keepdims=True)
    return centred * lax.rsqrt(row_var + LN_EPS) * ln_gain + ln_bias


def region_mask(extent):
    positions = jnp.arange(extent)
    labels = (positions >= extent - WINDOW).astype(jnp.int32) + (positions >= extent - SHIFT).astype(jnp.int32)
    labels = labels.reshape(extent // WINDOW, WINDOW)
    return labels[:, :, None] != labels[:, None, :]


def rel_bias_table(cpb_w1, cpb_b1, cpb_w2):
    offsets = jnp.arange(-(WINDOW - 1), WINDOW).astype(jnp.float32)
    coords = jnp.sign(offsets) * jnp.log2(1.0 + 8.0 * jnp.abs(offsets) / (WINDOW - 1)) / 3.0
    hidden = jax.nn.relu(coords[:, None, None] * cpb_w1[0] + coords[None, :, None] * cpb_w1[1] + cpb_b1)
    cpb_table = jnp.dot(hidden.reshape(-1, hidden.shape[-1]), cpb_w2, preferred_element_type=jnp.float32)
    cpb_table = cpb_table.reshape(2 * WINDOW - 1, 2 * WINDOW - 1, -1)
    win_pos = jnp.arange(WINDOW)
    rel_idx = win_pos[:, None] - win_pos[None, :] + WINDOW - 1
    gathered = cpb_table[rel_idx[:, None, :, None], rel_idx[None, :, None, :]]
    return 16.0 * jax.nn.sigmoid(jnp.moveaxis(gathered, -1, 0))


def reference(x, w_qkv, q_bias, v_bias, logit_scale, cpb_w1, cpb_b1, cpb_w2, w_proj, b_proj, ln1_gain, ln1_bias, w_fc1, b_fc1, w_fc2, b_fc2, ln2_gain, ln2_bias):
    n_rows = HEIGHT // WINDOW
    n_cols = WIDTH // WINDOW
    shifted = jnp.roll(x, (-SHIFT, -SHIFT), axis=(1, 2))
    qkv_all = jnp.einsum('bhwc,cte->bhwte', shifted.astype(jnp.float32), w_qkv.astype(jnp.float32))
    win_shape = (BATCH * n_rows, WINDOW, n_cols, WINDOW, N_HEADS, HEAD_DIM)
    q_win = (qkv_all[:, :, :, 0] + q_bias.astype(jnp.float32)).astype(jnp.bfloat16).reshape(win_shape)
    k_win = qkv_all[:, :, :, 1].astype(jnp.bfloat16).reshape(win_shape)
    v_win = (qkv_all[:, :, :, 2] + v_bias.astype(jnp.float32)).astype(jnp.bfloat16).reshape(win_shape)
    row_mask = jnp.tile(region_mask(HEIGHT), (BATCH, 1, 1))
    col_mask = region_mask(WIDTH)
    rel_bias = rel_bias_table(cpb_w1, cpb_b1, cpb_w2)
    head_scale = jnp.exp(jnp.minimum(logit_scale, math.log(100.0)))

    def one_row(operands):
        q_row, k_row, v_row, row_part = operands
        q_val = q_row.astype(jnp.float32)
        k_val = k_row.astype(jnp.float32)
        qk_dots = jnp.einsum('iujnd,kulnd->unijkl', q_val, k_val)
        q_norm = jnp.maximum(jnp.sqrt(jnp.sum(q_val * q_val, axis=-1)), NORM_EPS)
        k_norm = jnp.maximum(jnp.sqrt(jnp.sum(k_val * k_val, axis=-1)), NORM_EPS)
        q_norm = jnp.transpose(q_norm, (1, 3, 0, 2))[:, :, :, :, None, None]
        k_norm = jnp.transpose(k_norm, (1, 3, 0, 2))[:, :, None, None, :, :]
        masked = row_part[None, None, :, None, :, None] | col_mask[:, None, None, :, None, :]
        logits = qk_dots / (q_norm * k_norm) * head_scale[:, None, None, None, None] + rel_bias + jnp.where(masked, -100.0, 0.0)
        attn_prob = jax.nn.softmax(logits, axis=(4, 5)).astype(jnp.bfloat16)
        out_row = jnp.einsum('unijkl,kulnd->iujnd', attn_prob.astype(jnp.float32), v_row.astype(jnp.float32))
        return out_row.astype(jnp.bfloat16)

    attn_out = lax.map(one_row, (q_win, k_win, v_win, row_mask)).reshape(BATCH, HEIGHT, WIDTH, CHANNELS)
    proj_out = (jnp.einsum('bhwe,ec->bhwc', attn_out.astype(jnp.float32), w_proj.astype(jnp.float32)) + b_proj.astype(jnp.float32)).astype(jnp.bfloat16)
    unshifted = jnp.roll(proj_out, (SHIFT, SHIFT), axis=(1, 2))
    resid_y = (x.astype(jnp.float32) + layer_norm(unshifted.astype(jnp.float32), ln1_gain, ln1_bias)).astype(jnp.bfloat16)
    hidden = jax.nn.gelu(jnp.einsum('bhwc,cf->bhwf', resid_y.astype(jnp.float32), w_fc1.astype(jnp.float32)) + b_fc1.astype(jnp.float32), approximate=False).astype(jnp.bfloat16)
    mlp_out = (jnp.einsum('bhwf,fc->bhwc', hidden.astype(jnp.float32), w_fc2.astype(jnp.float32)) + b_fc2.astype(jnp.float32)).astype(jnp.bfloat16)
    return (resid_y.astype(jnp.float32) + layer_norm(mlp_out.astype(jnp.float32), ln2_gain, ln2_bias)).astype(jnp.bfloat16)
```

```python
import functools
import math
import jax
import jax.numpy as jnp
from jax import lax
from jax.experimental import pallas as pl
from jax.experimental.pallas import tpu as pltpu
from jax.sharding import PartitionSpec as P

WIN = 16
C, U, Q = 1024, 512, 256
LOG2E = 1.4426950408889634
F32, BF16 = jnp.float32, jnp.bfloat16
MESH = pl.DeviceIdType.MESH
HALF = 12
EXTRA = 2
AHEAD = 8
NU = HALF + EXTRA
LAG = 2
NEG = -100.0 * LOG2E


def ln_rows(u, gain, bias):
    mean = jnp.mean(u, axis=-1, keepdims=True)
    c = u - mean
    var = jnp.mean(c * c, axis=-1, keepdims=True)
    return c * lax.rsqrt(var + 1e-5) * gain + bias


def kernel(x_ref, wq_in, wp_in, w1_in, w2_in, pack_in, e_ref, vec_ref,
           out_ref, halo_ref,
           wq, wp, w1, w2, pack, bias, xb, oT, sring, pring, yb, gb, mb, zb,
           hal_s, hal_r, wz_s, wz_r, wy_s, wy_r, wx_s, wx_r, ws_s, ws_r, pk_s, pk_r, own_s,
           xl, lw, ls, lr, zs, zr):
    dp, z, sp = lax.axis_index("dp"), lax.axis_index("tp"), lax.axis_index("sp")
    half = lax.rem(z, 2)
    end = (z == 0) | (z == 3)
    n = jnp.where(end, NU, HALF)
    k_me = dp * 4 + sp
    ynb, xnb, sib = lax.rem(sp + 2, 4), 1 - dp, sp + 1 - 2 * lax.rem(sp, 2)
    up_sp, dn_sp = lax.rem(sp + 1, 4), lax.rem(sp + 3, 4)
    mats = ((wq_in, wq, 128), (wp_in, wp, 32), (w1_in, w1, 128), (w2_in, w2, 128))

    def where_is(i):
        uu = jnp.where(i < HALF, i, i - EXTRA)
        hf = jnp.where(i < HALF, half, 1 - half)
        return hf * 3 + uu // 4, lax.rem(uu, 4)

    def cols(jj):
        return (pl.multiple_of(jj * 32 + 8, 8), pl.multiple_of(jj * 32 + 24, 8),
                pl.multiple_of(lax.rem(jj * 32 + 32, 128), 8))

    def halo_copies(i):
        b, jj = where_is(i)
        c0, c1, c2 = cols(jj)
        mk = lambda s, d, w: pltpu.make_async_remote_copy(
            src_ref=x_ref.at[b, pl.ds(0, 8), pl.ds(s, w)], dst_ref=halo_ref.at[i, :, pl.ds(d, w)],
            send_sem=hal_s.at[i], recv_sem=hal_r.at[i], device_id=(dp, z, dn_sp), device_id_type=MESH)
        return mk(c0, 0, 24), mk(c2, 24, 8)

    def halo_wait(i):
        return pltpu.make_async_remote_copy(
            src_ref=halo_ref.at[i], dst_ref=halo_ref.at[i], send_sem=hal_s.at[i], recv_sem=hal_r.at[i],
            device_id=(dp, z, dn_sp), device_id_type=MESH)

    def halo_start(i):
        for c in halo_copies(i):
            c.start()

    def piece(m, p, k):
        rows = mats[m][2]
        return mats[m][1].at[p, pl.ds(pl.multiple_of(k * rows, rows), rows)]

    def own_copy(m):
        return pltpu.make_async_copy(mats[m][0], mats[m][1].at[z], own_s.at[m])

    def z_copy(m, q):
        rows = mats[m][2]
        d = lax.rem(z + q, 4)
        return pltpu.make_async_remote_copy(
            src_ref=mats[m][0].at[pl.ds(pl.multiple_of(k_me * rows, rows), rows)], dst_ref=piece(m, z, k_me),
            send_sem=wz_s.at[m, q - 1], recv_sem=wz_r.at[m, q - 1], device_id=(dp, d, sp), device_id_type=MESH)

    def pk_copy(q):
        d = lax.rem(z + q, 4)
        return pltpu.make_async_remote_copy(
            src_ref=pack_in, dst_ref=pack.at[z], send_sem=pk_s.at[q - 1], recv_sem=pk_r.at[q - 1],
            device_id=(dp, d, sp), device_id_type=MESH)

    def fwd(m, q, k, ssem, rsem, dev):
        p = lax.rem(z + 4 - q, 4)
        ref = piece(m, p, k)
        return pltpu.make_async_remote_copy(src_ref=ref, dst_ref=ref, send_sem=ssem, recv_sem=rsem,
                                            device_id=dev, device_id_type=MESH)

    k_y = dp * 4 + ynb
    k_x = xnb * 4 + sp
    k_xy = xnb * 4 + ynb
    dev_s, dev_y, dev_x = (dp, z, sib), (dp, z, ynb), (xnb, z, sp)
    f_y = lambda m, q: fwd(m, q, k_me, wy_s.at[m, q - 1], wy_r.at[m, q - 1], dev_y)
    f_x = lambda m, q, a: fwd(m, q, (k_me, k_y)[a], wx_s.at[m, q - 1, a], wx_r.at[m, q - 1, a], dev_x)
    f_s = lambda m, q, a: fwd(m, q, (k_me, k_y, k_x, k_xy)[a], ws_s.at[m, q - 1, a], ws_r.at[m, q - 1, a], dev_s)

    def each_q(f):
        def body(q, c):
            f(q)
            return c
        lax.fori_loop(1, 4, body, 0)

    def stage1(m):
        def f(q):
            z_copy(m, q).wait_recv()
            f_x(m, q, 0).start()
            f_y(m, q).start()
            f_s(m, q, 0).start()
        each_q(f)

    def stage2(m):
        def f(q):
            f_y(m, q).wait_recv()
            f_x(m, q, 1).start()
            f_s(m, q, 1).start()
        each_q(f)

    def stage3(m):
        def f(q):
            f_x(m, q, 0).wait_recv()
            f_s(m, q, 2).start()
            f_x(m, q, 1).wait_recv()
            f_s(m, q, 3).start()
        each_q(f)

    def stage4(m):
        def f(q):
            for a in range(4):
                f_s(m, q, a).wait_recv()
        each_q(f)
        own_copy(m).wait()

    def drain_w(m):
        def f(q):
            z_copy(m, q).wait_send()
            f_y(m, q).wait_send()
            for a in range(2):
                f_x(m, q, a).wait_send()
            for a in range(4):
                f_s(m, q, a).wait_send()
        each_q(f)

    def x_copies(i):
        b, jj = where_is(i)
        c0, c1, c2 = cols(jj)
        sl = lax.rem(i, 2)
        own = lambda c, w: x_ref.at[b, pl.ds(8, 8), pl.ds(c, w)]
        hal = lambda c, w: halo_ref.at[i, :, pl.ds(c, w)]
        prs = ((own(c0, 16), xb.at[sl, 0, pl.ds(0, 8)]), (hal(0, 16), xb.at[sl, 0, pl.ds(8, 8)]),
               (own(c1, 8), xb.at[sl, 1, pl.ds(0, 8), pl.ds(0, 8)]), (hal(16, 8), xb.at[sl, 1, pl.ds(8, 8), pl.ds(0, 8)]),
               (own(c2, 8), xb.at[sl, 1, pl.ds(0, 8), pl.ds(8, 8)]), (hal(24, 8), xb.at[sl, 1, pl.ds(8, 8), pl.ds(8, 8)]))
        return [pltpu.make_async_copy(s, d, xl.at[sl]) for s, d in prs]

    def x_start(i):
        halo_wait(i).wait_recv()
        for c in x_copies(i):
            c.start()

    def x_wait(i):
        sl = lax.rem(i, 2)
        pltpu.make_async_copy(xb.at[sl], xb.at[sl], xl.at[sl]).wait()

    def z_local(i):
        b, jj = where_is(i)
        c0, c1, c2 = cols(jj)
        sl = lax.rem(i, 2)
        o = lambda c, w: out_ref.at[b, pl.ds(8, 8), pl.ds(c, w)]
        return [pltpu.make_async_copy(s, d, lw.at[sl]) for s, d in (
            (zb.at[sl, 0, pl.ds(0, 8)], o(c0, 16)),
            (zb.at[sl, 1, pl.ds(0, 8), pl.ds(0, 8)], o(c1, 8)),
            (zb.at[sl, 1, pl.ds(0, 8), pl.ds(8, 8)], o(c2, 8)))]

    def z_band(i):
        b, jj = where_is(i)
        c0, c1, c2 = cols(jj)
        sl = lax.rem(i, 2)
        o = lambda c, w: out_ref.at[b, pl.ds(0, 8), pl.ds(c, w)]
        return [pltpu.make_async_remote_copy(src_ref=s, dst_ref=d, send_sem=ls.at[sl], recv_sem=lr.at[i],
                                             device_id=(dp, z, up_sp), device_id_type=MESH) for s, d in (
            (zb.at[sl, 0, pl.ds(8, 8)], o(c0, 16)),
            (zb.at[sl, 1, pl.ds(8, 8), pl.ds(0, 8)], o(c1, 8)),
            (zb.at[sl, 1, pl.ds(8, 8), pl.ds(8, 8)], o(c2, 8)))]

    def z_local_wait(i):
        sl = lax.rem(i, 2)
        ref = zb.at[sl, 0]
        pltpu.make_async_copy(ref, ref, lw.at[sl]).wait()

    def band_waits(i):
        sl = lax.rem(i, 2)
        ref = halo_ref.at[i]
        return pltpu.make_async_remote_copy(src_ref=ref, dst_ref=ref, send_sem=ls.at[sl], recv_sem=lr.at[i],
                                            device_id=(dp, z, up_sp), device_id_type=MESH)

    def z_send(i, h, d):
        b, jj = where_is(i)
        c0, c1, c2 = cols(jj)
        dz = jnp.clip(z + 2 * d - 1, 0, 3)
        r = lambda c, w: out_ref.at[b, pl.ds(8 * h, 8), pl.ds(c, w)]
        return [pltpu.make_async_remote_copy(src_ref=r(c, w), dst_ref=r(c, w), send_sem=zs.at[d, h, i], recv_sem=zr.at[h, i],
                                             device_id=(dp, dz, sp), device_id_type=MESH) for c, w in ((c0, 24), (c2, 8))]

    def z_send_waits(i, h, d):
        ref = halo_ref.at[0]
        return pltpu.make_async_remote_copy(src_ref=ref, dst_ref=ref, send_sem=zs.at[d, h, i], recv_sem=zr.at[h, i],
                                            device_id=(dp, z, sp), device_id_type=MESH)

    def sends_to(i, d):
        even = lax.rem(i, 2) == 0
        main = i < HALF - EXTRA
        if d == 1:
            ok = ((z <= 1) & even) | ((z == 2) & main)
        else:
            ok = ((z >= 2) & jnp.logical_not(even)) | ((z == 1) & main)
        return ok & (i < HALF)

    def z_send_start(i, h):
        for d in range(2):
            @pl.when(sends_to(i, d))
            def _():
                for c in z_send(i, h, d):
                    c.start()

    def attention(i):
        sl = lax.rem(i, 2)
        _, jj = where_is(i)
        last = jnp.where(jj == 3, 1, 0)

        def group(g, carry):
            x = xb[sl].reshape(U, C)
            q = jnp.dot(x, wq[g, :, 0:Q], preferred_element_type=F32) + pack[g, 1:2, 0:Q]
            k = jnp.dot(x, wq[g, :, Q:U], preferred_element_type=F32)
            v = jnp.dot(x, wq[g, :, U:768], preferred_element_type=F32) + pack[g, 1:2, Q:U]
            qT = q.astype(BF16).T
            kb = k.astype(BF16)
            vT = v.astype(BF16).T
            qf = qT.astype(F32).reshape(8, 32, U)
            kf = kb.T.astype(F32).reshape(8, 32, U)
            qs = pack[g, 8:16, 0:U] / jnp.maximum(jnp.sqrt(jnp.sum(qf * qf, axis=1)), 1e-12)
            ki = (1.0 / jnp.maximum(jnp.sqrt(jnp.sum(kf * kf, axis=1)), 1e-12)).T
            hw = [(h, w) for h in range(8) for w in range(2)]
            rs = {}

            def scores(t):
                h, w = hw[t]
                ts = slice(w * Q, w * Q + Q)
                parts = [jnp.zeros((32 * h, Q), BF16)] if h else []
                parts.append(qT[32 * h:32 * h + 32, ts])
                if h < 7:
                    parts.append(jnp.zeros((224 - 32 * h, Q), BF16))
                sring[t % (LAG + 1)] = jnp.dot(kb[ts, :], jnp.concatenate(parts, axis=0), preferred_element_type=F32)

            def soft(t):
                h, w = hw[t]
                ts = slice(w * Q, w * Q + Q)
                tab = bias[last, g * 8 + h] if w else bias[0, g * 8 + h]
                a = sring[t % (LAG + 1)] * ki[ts, h:h + 1] * qs[h:h + 1, ts] + tab
                e = jnp.exp2(a - jnp.max(a, axis=0, keepdims=True))
                rs[t] = 1.0 / jnp.sum(e, axis=0, keepdims=True)
                pring[t % (2 * LAG + 2)] = e.astype(BF16)

            def values(t):
                h, w = hw[t]
                ts = slice(w * Q, w * Q + Q)
                o = jnp.dot(vT[32 * h:32 * h + 32, ts], pring[t % (2 * LAG + 2)], preferred_element_type=F32)
                oT[pl.ds(pl.multiple_of(g * Q + 32 * h, 32), 32), ts] = (o * rs[t]).astype(BF16)

            for t in range(16 + 2 * LAG):
                if t < 16:
                    scores(t)
                if LAG <= t < 16 + LAG:
                    soft(t - LAG)
                if t >= 2 * LAG:
                    values(t - 2 * LAG)
            return carry
        lax.fori_loop(0, 4, group, 0)

    def project(i):
        sl = lax.rem(i, 2)
        ys = lax.rem(i, AHEAD)
        o = oT[...].T
        for nb in range(4):
            cs = slice(nb * Q, nb * Q + Q)
            acc = jnp.dot(o[:, 0:Q], wp[0, :, cs], preferred_element_type=F32)
            for p in range(1, 4):
                acc += jnp.dot(o[:, Q * p:Q * p + Q], wp[p, :, cs], preferred_element_type=F32)
            gb[:, cs] = (acc + vec_ref[0:1, cs]).astype(BF16)
        x = xb[sl].reshape(U, C).astype(F32)
        yb[ys] = (x + ln_rows(gb[...].astype(F32), vec_ref[1:2], vec_ref[2:3])).astype(BF16)

    def mlp(i):
        sl = lax.rem(i, 2)
        ys = lax.rem(i, AHEAD)
        mb[...] = jnp.zeros_like(mb)

        def part(s, carry):
            y = yb[ys]
            for nb in range(4):
                cs = slice(nb * Q, nb * Q + Q)
                h = jnp.dot(y, w1[s, :, cs], preferred_element_type=F32) + pack[s, 0:1, cs]
                gb[:, cs] = (0.5 * h * (1.0 + lax.erf(h * math.sqrt(0.5)))).astype(BF16)
            gg = gb[...]
            for nb in range(4):
                cs = slice(nb * Q, nb * Q + Q)
                mb[:, cs] += jnp.dot(gg, w2[s, :, cs], preferred_element_type=F32)
            return carry
        lax.fori_loop(0, 4, part, 0)
        u = (mb[...] + vec_ref[3:4]).astype(BF16).astype(F32)
        zz = (yb[ys].astype(F32) + ln_rows(u, vec_ref[4:5], vec_ref[5:6])).astype(BF16)
        zb[sl] = zz.reshape(2, 16, 16, C)

    def build_bias():
        rm = jnp.where(sp == 3, NEG, 0.0)
        kr = lax.broadcasted_iota(jnp.int32, (16, Q), 0)
        ql = lax.broadcasted_iota(jnp.int32, (16, Q), 1)
        cm = jnp.where((kr < 8) != (lax.rem(ql, 16) < 8), NEG, 0.0)
        top = jnp.where(ql >= 128, rm, 0.0)
        bot = jnp.where(ql < 128, rm, 0.0)

        def head(h, carry):
            e = e_ref[h]
            for ik in range(16):
                off = (15 - ik) * 16
                r = (pltpu.roll(e, U - off, 1) if off else e)[:, 0:Q]
                r = r + (top if ik < 8 else bot)
                bias[0, h, 16 * ik:16 * ik + 16, :] = r
                bias[1, h, 16 * ik:16 * ik + 16, :] = r + cm
            return carry
        lax.fori_loop(0, 32, head, 0)

    for i in range(2):
        halo_start(i)
    for m in range(4):
        own_copy(m).start()
    pk_own = pltpu.make_async_copy(pack_in, pack.at[z], own_s.at[4])
    pk_own.start()
    each_q(lambda q: pk_copy(q).start())
    for m in range(4):
        each_q(lambda q: z_copy(m, q).start())
    x_start(0)
    build_bias()
    stage1(0)
    stage2(0)
    stage1(1)
    stage3(0)
    stage2(1)
    stage4(0)
    each_q(lambda q: pk_copy(q).wait_recv())
    pk_own.wait()

    def tick(t, carry):
        @pl.when(t == 0)
        def _():
            stage3(1)
            stage1(2)

        @pl.when(t == 1)
        def _():
            stage2(2)

        @pl.when(t == 3)
        def _():
            stage1(3)

        @pl.when(t == 4)
        def _():
            stage3(2)
            stage2(3)

        @pl.when(t == 6)
        def _():
            stage4(2)
            stage3(3)

        @pl.when(t == AHEAD)
        def _():
            stage4(3)

        m = t - AHEAD

        @pl.when(m >= 2)
        def _():
            band_waits(m - 2).wait_send()
            band_waits(m - 2).wait_recv()
            z_send_start(m - 2, 0)

        @pl.when(m >= 0)
        def _():
            mlp(m)
            for c in z_local(m):
                c.start()
            for c in z_band(m):
                c.start()

        @pl.when(m >= 1)
        def _():
            z_local_wait(m - 1)
            z_send_start(m - 1, 1)

        @pl.when(t + 2 < n)
        def _():
            halo_start(t + 2)

        @pl.when(t < n)
        def _():
            x_wait(t)

            @pl.when(t + 1 < n)
            def _():
                x_start(t + 1)
            attention(t)

        @pl.when(t == 0)
        def _():
            stage4(1)

        @pl.when(t < n)
        def _():
            project(t)
        return carry
    lax.fori_loop(0, n + AHEAD, tick, 0)

    def tail(i, carry):
        band_waits(i).wait_send()
        band_waits(i).wait_recv()
        z_send_start(i, 0)
        return carry
    lax.fori_loop(n - 2, n, tail, 0)
    z_local_wait(n - 1)
    z_send_start(n - 1, 1)

    def drain(i, carry):
        halo_wait(i).wait_send()
        for h in range(2):
            for d in range(2):
                @pl.when(sends_to(i, d))
                def _():
                    z_send_waits(i, h, d).wait_send()
        return carry
    lax.fori_loop(0, n, drain, 0)
    for m in range(4):
        drain_w(m)
    each_q(lambda q: pk_copy(q).wait_send())

    def arrive(i, carry):
        for h in range(2):
            z_send_waits(i, h, 0).wait_recv()
        return carry
    lax.fori_loop(0, jnp.where(end, HALF - EXTRA, HALF), arrive, 0)


def block(x, wq, wp, w1, w2, pack, etab, vec):
    hbm = pl.BlockSpec(memory_space=pl.ANY)
    vm = pl.BlockSpec(memory_space=pltpu.VMEM)
    dma = pltpu.SemaphoreType.DMA
    out, _ = pl.pallas_call(
        kernel, name="swin",
        out_shape=(jax.ShapeDtypeStruct(x.shape, BF16), jax.ShapeDtypeStruct((NU, 8, 32, C), BF16)),
        in_specs=[hbm] * 6 + [vm] * 2, out_specs=(hbm, hbm),
        scratch_shapes=[
            pltpu.VMEM((4, C, 768), BF16), pltpu.VMEM((4, Q, C), BF16),
            pltpu.VMEM((4, C, C), BF16), pltpu.VMEM((4, C, C), BF16),
            pltpu.VMEM((4, 16, C), F32), pltpu.VMEM((2, 32, Q, Q), F32),
            pltpu.VMEM((2, 2, 16, 16, C), BF16), pltpu.VMEM((C, U), BF16),
            pltpu.VMEM((LAG + 1, Q, Q), F32), pltpu.VMEM((2 * LAG + 2, Q, Q), BF16),
            pltpu.VMEM((AHEAD, U, C), BF16), pltpu.VMEM((U, C), BF16), pltpu.VMEM((U, C), F32),
            pltpu.VMEM((2, 2, 16, 16, C), BF16),
            dma((NU,)), dma((NU,)), dma((4, 3)), dma((4, 3)), dma((4, 3)), dma((4, 3)),
            dma((4, 3, 2)), dma((4, 3, 2)), dma((4, 3, 4)), dma((4, 3, 4)), dma((3,)), dma((3,)), dma((5,)),
            dma((2,)), dma((2,)), dma((2,)), dma((NU,)), dma((2, 2, NU)), dma((2, HALF))],
        compiler_params=pltpu.CompilerParams(has_side_effects=True, vmem_limit_bytes=67_000_000),
    )(x, wq, wp, w1, w2, pack, etab, vec)
    return out


def solution(mesh):
    def block_fn(x, w_qkv, q_bias, v_bias, logit_scale, cpb_w1, cpb_b1, cpb_w2, w_proj, b_proj, g1, be1, w_fc1, b_fc1, w_fc2, b_fc2, g2, be2):
        hs = jnp.exp(jnp.minimum(logit_scale, math.log(100.0))) * LOG2E
        pack = jnp.concatenate([
            b_fc1.astype(F32)[None], jnp.concatenate([q_bias.astype(F32), v_bias.astype(F32), jnp.zeros((U,), F32)])[None],
            jnp.zeros((6, C), F32), jnp.broadcast_to(hs[:, None], (8, C))], axis=0)
        vec = jnp.stack([b_proj.astype(F32), g1, be1, b_fc2.astype(F32), g2, be2, jnp.zeros_like(g1), jnp.zeros_like(g1)])
        offs = jnp.arange(-(WIN - 1), WIN).astype(F32)
        co = jnp.sign(offs) * jnp.log2(1.0 + 8.0 * jnp.abs(offs) / (WIN - 1)) / 3.0
        hid = jax.nn.relu(co[:, None, None] * cpb_w1[0] + co[None, :, None] * cpb_w1[1] + cpb_b1)
        tab = jnp.dot(hid.reshape(-1, hid.shape[-1]), cpb_w2, precision=lax.Precision.HIGHEST, preferred_element_type=F32)
        tab = (16.0 * LOG2E) * jax.nn.sigmoid(tab.T.reshape(32, 31, 31))
        et = jnp.stack([tab[:, :, 15 - j:31 - j] for j in range(16)], axis=1).reshape(32, 16, 496)
        et = jnp.pad(et, ((0, 0), (0, 0), (0, 16)))
        return block(x, w_qkv.reshape(C, 768), w_proj, w_fc1, w_fc2, pack, et, vec)

    band = P('dp', 'sp', None, None)
    whole = P(None)
    in_specs = (band, P(None, None, 'tp'), P('tp'), P('tp'), P('tp'), P(None, None), whole, P(None, None), P('tp', None), whole, whole, whole, P(None, 'tp'), P('tp'), P('tp', None), whole, whole, whole)
    return jax.shard_map(block_fn, mesh=mesh, in_specs=in_specs, out_specs=band, check_vma=False)
```

```python
import functools
import math
import jax
import jax.numpy as jnp
from jax import lax
from jax.experimental import pallas as pl
from jax.experimental.pallas import tpu as pltpu
from jax.sharding import PartitionSpec as P

WIN = 16
C, U, Q = 1024, 512, 256
LOG2E = 1.4426950408889634
N3, N4, N6, S8, W24, D, LN = 3, 4, 6, 8, 24, 32, 128
F32, BF16 = jnp.float32, jnp.bfloat16
MESH = pl.DeviceIdType.MESH
HALF = 12
EXTRA = 1
AHEAD = 6
NU = HALF + EXTRA
LAG = N4
NEG = -100.0 * LOG2E


def ln_rows(u, gain, bias):
    mean = jnp.mean(u, axis=-1, keepdims=True)
    c = u - mean
    var = jnp.mean(c * c, axis=-1, keepdims=True)
    return c * lax.rsqrt(var + 1e-5) * gain + bias


def kernel(x_ref, wq_in, wp_in, w1_in, w2_in, pack_in, cw1, cb1, cw2, bp, g1, be1, b2, g2, be2,
           out_ref, halo_ref,
           wq, wp, w1, w2, pack, bias, cmask, xb, oT, pring, qTs, kbs, vTs, qss, kis, ub, yb, gb, mb, zb,
           hal_s, hal_r, wz_s, wz_r, wy_s, wy_r, wx_s, wx_r, ws_s, ws_r, pk_s, pk_r, own_s,
           xl, lw, ls, lr, zs, zr):
    dp, z, sp = lax.axis_index("dp"), lax.axis_index("tp"), lax.axis_index("sp")
    half = lax.rem(z, 2)
    end = (z == 0) | (z == N3)
    n = jnp.where(end, NU, HALF)
    k_me = dp * N4 + sp
    ynb, xnb, sib = lax.rem(sp + 2, N4), 1 - dp, sp + 1 - 2 * lax.rem(sp, 2)
    up_sp, dn_sp = lax.rem(sp + 1, N4), lax.rem(sp + N3, N4)
    mats = ((wq_in, wq, LN), (wp_in, wp, D), (w1_in, w1, LN), (w2_in, w2, LN))
    rng = lambda m, k: pl.ds(pl.multiple_of(k * mats[m][2], mats[m][2]), mats[m][2])
    cut = lambda ref, m, k: ref.at[:, rng(m, k)] if m == 0 else ref.at[rng(m, k)]

    def where_is(i):
        uu = jnp.where(i < HALF, i, i - EXTRA)
        hf = jnp.where(i < HALF, half, 1 - half)
        return hf * N3 + uu // N4, lax.rem(uu, N4)

    def cols(jj):
        return (pl.multiple_of(jj * D + S8, S8), pl.multiple_of(jj * D + W24, S8),
                pl.multiple_of(lax.rem(jj * D + D, LN), S8))

    def halo_copies(i):
        b, jj = where_is(i)
        c0, c1, c2 = cols(jj)
        mk = lambda s, d, w: pltpu.make_async_remote_copy(
            src_ref=x_ref.at[b, pl.ds(0, S8), pl.ds(s, w)], dst_ref=halo_ref.at[i, :, pl.ds(d, w)],
            send_sem=hal_s.at[i], recv_sem=hal_r.at[i], device_id=(dp, z, dn_sp), device_id_type=MESH)
        return mk(c0, 0, W24), mk(c2, W24, S8)

    def halo_wait(i):
        return pltpu.make_async_remote_copy(
            src_ref=halo_ref.at[i], dst_ref=halo_ref.at[i], send_sem=hal_s.at[i], recv_sem=hal_r.at[i],
            device_id=(dp, z, dn_sp), device_id_type=MESH)

    def halo_start(i):
        for c in halo_copies(i):
            c.start()

    def piece(m, p, k):
        return cut(mats[m][1].at[p], m, k)

    def own_copy(m):
        return pltpu.make_async_copy(mats[m][0], mats[m][1].at[z], own_s.at[m])

    def remote(src, dst, ssem, rsem, dev):
        return pltpu.make_async_remote_copy(src_ref=src, dst_ref=dst, send_sem=ssem, recv_sem=rsem,
                                            device_id=dev, device_id_type=MESH)

    def shard(i):
        near = jnp.where(z == 0, 1, z - 1)
        next_ = jnp.where(z == 0, 2, jnp.where(z == N3, 1, z + 1))
        return jnp.where(i == 0, near, jnp.where(i == 1, next_, jnp.where(z < 2, N3, 0)))

    k_y = dp * N4 + ynb
    k_x = xnb * N4 + sp
    k_xy = xnb * N4 + ynb
    ks = (k_me, k_y, k_x, k_xy)
    dev_s, dev_y, dev_x = (dp, z, sib), (dp, z, ynb), (xnb, z, sp)
    def z_own(m, q):
        return remote(cut(mats[m][0], m, k_me), piece(m, z, k_me), wz_s.at[m, q - 1], wz_r.at[m, z],
                      (dp, lax.rem(z + q, N4), sp))

    def z_came(m, p):
        ref = piece(m, p, k_me)
        return remote(ref, ref, wz_s.at[m, 0], wz_r.at[m, p], (dp, z, sp))

    def pk_copy(q):
        return remote(pack_in, pack.at[z], pk_s.at[q - 1], pk_r.at[q - 1], (dp, lax.rem(z + q, N4), sp))

    def fwd(m, p, a, sems, b, dev):
        ref = piece(m, p, ks[a])
        return remote(ref, ref, sems[0].at[m, p, b], sems[1].at[m, p, b], dev)

    f_y = lambda m, p, b: fwd(m, p, (0, 2)[b], (wy_s, wy_r), b, dev_y)
    f_x = lambda m, p, b: fwd(m, p, (0, 1)[b], (wx_s, wx_r), b, dev_x)
    f_s = lambda m, p, a: fwd(m, p, a, (ws_s, ws_r), a, dev_s)

    def each_q(f):
        def body(q, c):
            f(q)
            return c
        lax.fori_loop(1, N4, body, 0)

    def via(m, i):
        return ("xyx", "xxx", "xxx", "xyx")[m][i]

    def relay1(m, i):
        p = shard(i)
        z_came(m, p).wait_recv()
        f_x(m, p, 0).start()
        f_y(m, p, 0).start()
        f_s(m, p, 0).start()

    def relay2(m, i):
        p = shard(i)
        f_y(m, p, 0).wait_recv()
        if via(m, i) == "x":
            f_x(m, p, 1).start()
        f_s(m, p, 1).start()

    def relay3(m, i):
        p = shard(i)
        f_x(m, p, 0).wait_recv()
        if via(m, i) == "y":
            f_y(m, p, 1).start()
        f_s(m, p, 2).start()

    def relay4(m, i):
        p = shard(i)
        (f_x if via(m, i) == "x" else f_y)(m, p, 1).wait_recv()
        f_s(m, p, N3).start()

    def arrived(m):
        def f(q):
            p = shard(q - 1)
            for a in range(N4):
                f_s(m, p, a).wait_recv()
        each_q(f)
        own_copy(m).wait()

    def drain_w(m):
        each_q(lambda q: z_own(m, q).wait_send())
        for i in range(N3):
            p = shard(i)
            f_y(m, p, 0).wait_send()
            f_x(m, p, 0).wait_send()
            if via(m, i) == "x":
                f_x(m, p, 1).wait_send()
            if via(m, i) == "y":
                f_y(m, p, 1).wait_send()
            for a in range(N4):
                f_s(m, p, a).wait_send()

    def x_copies(i):
        b, jj = where_is(i)
        c0, c1, c2 = cols(jj)
        sl = lax.rem(i, N4)
        own = lambda c, w: x_ref.at[b, pl.ds(S8, S8), pl.ds(c, w)]
        hal = lambda c, w: halo_ref.at[i, :, pl.ds(c, w)]
        prs = ((own(c0, 16), xb.at[sl, 0, pl.ds(0, S8)]), (hal(0, 16), xb.at[sl, 0, pl.ds(S8, S8)]),
               (own(c1, S8), xb.at[sl, 1, pl.ds(0, S8), pl.ds(0, S8)]), (hal(16, S8), xb.at[sl, 1, pl.ds(S8, S8), pl.ds(0, S8)]),
               (own(c2, S8), xb.at[sl, 1, pl.ds(0, S8), pl.ds(S8, S8)]), (hal(W24, S8), xb.at[sl, 1, pl.ds(S8, S8), pl.ds(S8, S8)]))
        return [pltpu.make_async_copy(s, d, xl.at[sl]) for s, d in prs]

    def x_start(i):
        halo_wait(i).wait_recv()
        for c in x_copies(i):
            c.start()

    def x_wait(i):
        sl = lax.rem(i, N4)
        pltpu.make_async_copy(xb.at[sl], xb.at[sl], xl.at[sl]).wait()

    def z_local(i):
        b, jj = where_is(i)
        c0, c1, c2 = cols(jj)
        sl = lax.rem(i, 2)
        o = lambda c, w: out_ref.at[b, pl.ds(S8, S8), pl.ds(c, w)]
        return [pltpu.make_async_copy(s, d, lw.at[sl]) for s, d in (
            (zb.at[sl, 0, pl.ds(0, S8)], o(c0, 16)),
            (zb.at[sl, 1, pl.ds(0, S8), pl.ds(0, S8)], o(c1, S8)),
            (zb.at[sl, 1, pl.ds(0, S8), pl.ds(S8, S8)], o(c2, S8)))]

    def z_band(i):
        b, jj = where_is(i)
        c0, c1, c2 = cols(jj)
        sl = lax.rem(i, 2)
        o = lambda c, w: out_ref.at[b, pl.ds(0, S8), pl.ds(c, w)]
        return [pltpu.make_async_remote_copy(src_ref=s, dst_ref=d, send_sem=ls.at[sl], recv_sem=lr.at[i],
                                             device_id=(dp, z, up_sp), device_id_type=MESH) for s, d in (
            (zb.at[sl, 0, pl.ds(S8, S8)], o(c0, 16)),
            (zb.at[sl, 1, pl.ds(S8, S8), pl.ds(0, S8)], o(c1, S8)),
            (zb.at[sl, 1, pl.ds(S8, S8), pl.ds(S8, S8)], o(c2, S8)))]

    def z_local_wait(i):
        sl = lax.rem(i, 2)
        ref = zb.at[sl, 0]
        pltpu.make_async_copy(ref, ref, lw.at[sl]).wait()

    def band_waits(i):
        sl = lax.rem(i, 2)
        ref = halo_ref.at[i]
        return pltpu.make_async_remote_copy(src_ref=ref, dst_ref=ref, send_sem=ls.at[sl], recv_sem=lr.at[i],
                                            device_id=(dp, z, up_sp), device_id_type=MESH)

    def z_send(i, h, d):
        b, jj = where_is(i)
        c0, c1, c2 = cols(jj)
        dz = jnp.clip(z + 2 * d - 1, 0, N3)
        r = lambda c, w: out_ref.at[b, pl.ds(S8 * h, S8), pl.ds(c, w)]
        return [pltpu.make_async_remote_copy(src_ref=r(c, w), dst_ref=r(c, w), send_sem=zs.at[d, h, i], recv_sem=zr.at[h, i],
                                             device_id=(dp, dz, sp), device_id_type=MESH) for c, w in ((c0, W24), (c2, S8))]

    def z_send_waits(i, h, d):
        ref = halo_ref.at[0]
        return pltpu.make_async_remote_copy(src_ref=ref, dst_ref=ref, send_sem=zs.at[d, h, i], recv_sem=zr.at[h, i],
                                            device_id=(dp, z, sp), device_id_type=MESH)

    def sends_to(i, d):
        even = lax.rem(i, 2) == 0
        main = i < HALF - EXTRA
        if d == 1:
            ok = ((z <= 1) & even) | ((z == 2) & main)
        else:
            ok = ((z >= 2) & jnp.logical_not(even)) | ((z == 1) & main)
        return ok & (i < HALF)

    def z_send_start(i, h):
        for d in range(2):
            @pl.when(sends_to(i, d))
            def _():
                for c in z_send(i, h, d):
                    c.start()

    dot = lambda a, b: jnp.dot(a, b, preferred_element_type=F32)
    blk = lambda j: slice(j * Q, j * Q + Q)

    def queries(t, g, sl):
        x = lambda: xb[lax.rem(t, N4)].reshape(U, C)
        sq = lambda a: jnp.maximum(jnp.sqrt(jnp.sum(a * a, axis=1)), 1e-12)
        qT = (dot(x(), wq[g, 0]) + pack[g, 1:2, 0:Q]).astype(BF16).T
        qTs[sl] = qT
        qss[sl] = pack[g, S8:16, 0:U] / sq(qT.astype(F32).reshape(S8, D, U))
        kb = dot(x(), wq[g, 1]).astype(BF16)
        kbs[sl] = kb
        kis[sl] = (1.0 / sq(kb.T.astype(F32).reshape(S8, D, U))).T
        vTs[sl] = (dot(x(), wq[g, 2]) + pack[g, 1:2, Q:U]).astype(BF16).T

    def attention(t, g, sl):
        _, jj = where_is(t)
        last = jnp.where(jj == N3, NEG, 0.0)
        par = lax.rem(t, 2)
        hw = [(h, w) for h in range(S8) for w in range(2)]
        rs = {}

        def soft(i):
            h, w = hw[i]
            ts = blk(w)
            parts = [jnp.zeros((D * h, Q), BF16)] if h else []
            parts.append(qTs[sl, D * h:D * h + D, ts])
            if h < 7:
                parts.append(jnp.zeros((224 - D * h, Q), BF16))
            a = dot(kbs[sl, ts, :], jnp.concatenate(parts, axis=0))
            a = a * kis[sl, ts, h:h + 1] * qss[sl, h:h + 1, ts] + bias[g * S8 + h]
            if w:
                a = (a.reshape(WIN, WIN, Q) + (cmask[...] * last)[None]).reshape(Q, Q)
            e = jnp.exp2(a - jnp.max(a, axis=0, keepdims=True))
            rs[i] = 1.0 / jnp.sum(e, axis=0, keepdims=True)
            pring[i % (LAG + 2)] = e.astype(BF16)

        def values(i):
            h, w = hw[i]
            o = dot(vTs[sl, D * h:D * h + D, blk(w)], pring[i % (LAG + 2)])
            oT[par, pl.ds(pl.multiple_of(g * Q + D * h, D), D), blk(w)] = (o * rs[i]).astype(BF16)

        for i in range(WIN + LAG):
            if i < WIN:
                soft(i)
            if i >= LAG:
                values(i - LAG)

    def project(t, g):
        r = pl.ds(pl.multiple_of(g * LN, LN), LN)
        o = oT[lax.rem(t, 2), :, r].T
        for nb in range(N4):
            acc = dot(o[:, blk(0)], wp[0, :, blk(nb)])
            for p in range(1, N4):
                acc += dot(o[:, blk(p)], wp[p, :, blk(nb)])
            ub[:, blk(nb)] = (acc + bp[:, blk(nb)].astype(F32)).astype(BF16)

    def norm1(t, g):
        r = pl.ds(pl.multiple_of(g * LN, LN), LN)
        x = xb[lax.rem(t, N4), g // 2, pl.ds(pl.multiple_of(lax.rem(g, 2) * S8, S8), S8)].reshape(LN, C).astype(F32)
        yb[lax.rem(t, AHEAD), r] = (x + ln_rows(ub[...].astype(F32), g1[...], be1[...])).astype(BF16)

    def up(m, s):
        y = lambda: yb[lax.rem(m, AHEAD)]
        for nb in range(N4):
            h = dot(y(), w1[s, :, blk(nb)]) + pack[s, 0:1, blk(nb)]
            gb[:, blk(nb)] = (0.5 * h * (1.0 + lax.erf(h * math.sqrt(0.5)))).astype(BF16)

    def down(m, s):
        for nb in range(N4):
            mb[lax.rem(m, 2), :, blk(nb)] += dot(gb[...], w2[s, :, blk(nb)])

    def clear(m):
        mb[lax.rem(m, 2)] = jnp.broadcast_to(b2[...].astype(F32), (U, C))

    def norm2(m, g):
        sl = lax.rem(m + 2, 2)
        r = pl.ds(pl.multiple_of(g * LN, LN), LN)
        u = mb[sl, r].astype(BF16).astype(F32)
        zz = yb[lax.rem(m + AHEAD, AHEAD), r].astype(F32) + ln_rows(u, g2[...], be2[...])
        zb[sl, g // 2, pl.ds(pl.multiple_of(lax.rem(g, 2) * S8, S8), S8)] = zz.astype(BF16).reshape(S8, WIN, C)

    def build_bias():
        rm = jnp.where(sp == N3, NEG, 0.0)
        ql = lax.broadcasted_iota(jnp.int32, (WIN, Q), 1)
        kr = lax.broadcasted_iota(jnp.int32, (WIN, Q), 0)
        cmask[...] = jnp.where((kr < S8) != (lax.rem(ql, WIN) < S8), 1.0, 0.0)
        top = jnp.where(ql >= LN, rm, 0.0)
        bot = jnp.where(ql < LN, rm, 0.0)
        for part in range(N4):
            row = lax.broadcasted_iota(jnp.int32, (Q, LN), 0) + part * Q

            def coord(d):
                far = jnp.log(1.0 + (8.0 / (WIN - 1)) * jnp.abs(d).astype(F32)) * (LOG2E / 3.0)
                return jnp.concatenate([jnp.where(d < 0, -far, far)] * N4, axis=1)
            hid = coord(row // D - 15) * cw1[0:1] + coord(lax.rem(row, D) - 15) * cw1[1:2] + cb1[...]
            tab = lax.dot_general(cw2[...], jnp.maximum(hid, 0.0), (((1,), (1,)), ((), ())),
                                  precision=lax.Precision.HIGHEST, preferred_element_type=F32)
            mb[0, 0:D, blk(part)] = (WIN * LOG2E) / (1.0 + jnp.exp(-tab))
        row = lax.broadcasted_iota(jnp.int32, (U, Q), 0)
        col = lax.broadcasted_iota(jnp.int32, (U, Q), 1)
        pick = (row // D == col // WIN) & (lax.rem(row, D) == lax.rem(col, WIN))
        gb[:, 0:Q] = jnp.where(pick, 1.0, 0.0).astype(BF16)

        def head(h, carry):
            r = pltpu.roll(jnp.broadcast_to(mb[0, pl.ds(h, 1), :], (WIN, C)), C - 15, 1, stride=1, stride_axis=0)
            terms = []
            for _ in range(N3):
                terms.append(r.astype(BF16))
                r = r - terms[-1].astype(F32)
            terms = jnp.concatenate(terms, axis=0)
            e = []
            for k in range(2):
                p = dot(terms[:, k * U:k * U + U], gb[:, 0:Q])
                e.append(p[0:WIN] + p[WIN:2 * WIN] + p[2 * WIN:])
            e = jnp.concatenate(e, axis=1)
            for ik in range(WIN):
                off = (15 - ik) * WIN
                r = (pltpu.roll(e, U - off, 1) if off else e)[:, 0:Q]
                bias[h, WIN * ik:WIN * ik + WIN, :] = r + (top if ik < S8 else bot)
            return carry
        lax.fori_loop(0, D, head, 0)

    def each_g(f):
        def it(g, carry):
            f(g)
            return carry
        lax.fori_loop(0, N4, it, 0)

    halo_start(0)
    for m in range(N4):
        own_copy(m).start()
    pk_own = pltpu.make_async_copy(pack_in, pack.at[z], own_s.at[N4])
    pk_own.start()
    each_q(lambda q: z_own(0, q).start())
    each_q(lambda q: pk_copy(q).start())
    x_start(0)
    build_bias()
    relay1(0, 0)
    relay1(0, 1)
    each_q(lambda q: z_own(1, q).start())
    relay2(0, 0)
    relay3(0, 0)
    relay1(0, 2)
    each_q(lambda q: z_own(2, q).start())
    relay2(0, 1)
    relay3(0, 1)
    halo_start(1)
    relay4(0, 0)
    relay2(0, 2)
    relay3(0, 2)
    for i in range(N3):
        relay1(1, i)
    relay4(0, 1)
    for i in range(N3):
        relay2(1, i)
    relay4(0, 2)
    halo_start(2)
    arrived(0)
    each_q(lambda q: pk_copy(q).wait_recv())
    pk_own.wait()
    x_start(1)
    x_wait(0)
    queries(0, 0, 0)

    def service(j):
        @pl.when(j == 1)
        def _():
            each_q(lambda q: z_own(N3, q).start())

        for first, step, f, m in ((1, 1, relay1, 2), (1, 1, relay3, 1), (1, 1, relay4, 1), (5, 1, relay3, 2), (5, 1, relay2, 2),
                                  (7, 1, relay1, N3), (11, 1, relay4, 2), (11, 1, relay2, N3), (14, 1, relay3, N3), (16, 1, relay4, N3)):
            for i in range(N3):
                @pl.when(j == first + i * step)
                def _():
                    f(m, i)

    def pass_on(u, g):
        @pl.when((g == 1) & (u >= 0))
        def _():
            z_local_wait(u)
            z_send_start(u, 1)

        @pl.when((g == N3) & (u >= 0))
        def _():
            band_waits(u).wait_recv()
            z_send_start(u, 0)

    def after(u):
        @pl.when(u >= 0)
        def _():
            for c in z_local(u):
                c.start()
            for c in z_band(u):
                c.start()

    def next_x(t):
        @pl.when(t + 1 < n)
        def _():
            x_wait(t + 1)

        @pl.when(t + 2 < n)
        def _():
            x_start(t + 2)

        @pl.when(t + N3 < n)
        def _():
            halo_start(t + N3)

    def ask(t, g):
        queries(jnp.where(g == N3, jnp.minimum(t + 1, n - 1), t), lax.rem(g + 1, N4), lax.rem(g + 1, 2))

    def first(g):
        service(g)
        ask(0, g)
        attention(0, g, lax.rem(g, 2))
    next_x(0)
    each_g(first)
    arrived(1)

    def upto(t):
        return jnp.where(t < AHEAD - 1, 0, jnp.where(t < n, t - AHEAD + N3, n))

    def tick(t, carry):
        lo, hi = upto(t - 1), upto(t)

        @pl.when(t == AHEAD - 1)
        def _():
            arrived(2)
            arrived(N3)

        @pl.when(t == n)
        def _():
            def finish(g):
                project(n - 1, g)
                norm1(n - 1, g)
            each_g(finish)

        def mlp(m, c):
            @pl.when(m >= N3)
            def _():
                band_waits(m - N3).wait_send()
            clear(m)

            def it(g):
                pass_on(jnp.where(m > lo, m - 2, -1), g)
                up(m, g)
                norm2(m - 1, g)
                down(m, g)
            each_g(it)
            after(m - 1)
            return c
        lax.fori_loop(lo, hi, mlp, 0)

        @pl.when(t < n)
        def _():
            next_x(t)

            def it(g):
                service(N4 * t + g)
                pass_on(hi - 2, g)
                project(t - 1, g)
                ask(t, g)
                norm1(t - 1, g)
                attention(t, g, lax.rem(g, 2))
            each_g(it)
        return carry
    lax.fori_loop(1, n + 1, tick, 0)
    band_waits(n - N3).wait_send()

    def last(g):
        pass_on(n - 2, g)
        norm2(n - 1, g)
    each_g(last)
    after(n - 1)
    band_waits(n - 2).wait_send()
    z_local_wait(n - 1)
    z_send_start(n - 1, 1)
    band_waits(n - 1).wait_send()
    band_waits(n - 1).wait_recv()
    z_send_start(n - 1, 0)

    def drain(i, carry):
        halo_wait(i).wait_send()
        for h in range(2):
            for d in range(2):
                @pl.when(sends_to(i, d))
                def _():
                    z_send_waits(i, h, d).wait_send()
        return carry
    lax.fori_loop(0, n, drain, 0)
    for m in range(N4):
        drain_w(m)
    each_q(lambda q: pk_copy(q).wait_send())

    def arrive(i, carry):
        for h in range(2):
            z_send_waits(i, h, 0).wait_recv()
        return carry
    lax.fori_loop(0, jnp.where(end, HALF - EXTRA, HALF), arrive, 0)


def block(*args):
    hbm = pl.BlockSpec(memory_space=pl.ANY)
    vm = pl.BlockSpec(memory_space=pltpu.VMEM)
    dma, V = pltpu.SemaphoreType.DMA, pltpu.VMEM
    out, _ = pl.pallas_call(
        kernel, name="swin",
        out_shape=(jax.ShapeDtypeStruct(args[0].shape, BF16), jax.ShapeDtypeStruct((NU, S8, D, C), BF16)),
        in_specs=[hbm] * N6 + [vm] * 9, out_specs=(hbm, hbm),
        scratch_shapes=[
            V((N4, N3, C, Q), BF16), V((N4, Q, C), BF16), V((N4, C, C), BF16), V((N4, C, C), BF16), V((N4, WIN, C), F32),
            V((D, Q, Q), F32), V((WIN, Q), F32), V((N4, 2, WIN, WIN, C), BF16), V((2, C, U), BF16), V((LAG + 2, Q, Q), BF16),
            V((2, Q, U), BF16), V((2, U, Q), BF16), V((2, Q, U), BF16), V((2, S8, U), F32), V((2, U, S8), F32),
            V((LN, C), BF16), V((AHEAD, U, C), BF16), V((U, C), BF16), V((2, U, C), F32), V((2, 2, WIN, WIN, C), BF16),
            dma((NU,)), dma((NU,)), dma((N4, N3)), dma((N4, N4)), dma((N4, N4, 2)), dma((N4, N4, 2)),
            dma((N4, N4, 2)), dma((N4, N4, 2)), dma((N4, N4, N4)), dma((N4, N4, N4)), dma((N3,)), dma((N3,)), dma((5,)),
            dma((N4,)), dma((2,)), dma((2,)), dma((NU,)), dma((2, 2, NU)), dma((2, HALF))],
        compiler_params=pltpu.CompilerParams(has_side_effects=True, vmem_limit_bytes=67_000_000),
    )(*args)
    return out


def solution(mesh):
    def block_fn(x, w_qkv, q_bias, v_bias, logit_scale, cpb_w1, cpb_b1, cpb_w2, w_proj, b_proj, g1, be1, w_fc1, b_fc1, w_fc2, b_fc2, g2, be2):
        hs = jnp.exp(jnp.minimum(logit_scale, math.log(100.0))) * LOG2E
        r = lax.broadcasted_iota(jnp.int32, (WIN, C), 0)
        qv = jnp.pad(q_bias, (0, C - Q)).astype(F32) + jnp.pad(v_bias, (Q, U)).astype(F32)
        pack = jnp.where(r == 0, b_fc1.astype(F32)[None], jnp.where(r == 1, qv[None], jnp.pad(hs, (S8, 0))[:, None]))
        row = lambda a: a.reshape(1, -1)
        return block(x, w_qkv.transpose(1, 0, 2), w_proj, w_fc1, w_fc2, pack, cpb_w1, row(cpb_b1), cpb_w2.T,
                     row(b_proj), row(g1), row(be1), row(b_fc2), row(g2), row(be2))

    band = P('dp', 'sp', None, None)
    whole = P(None)
    in_specs = (band, P(None, None, 'tp'), P('tp'), P('tp'), P('tp'), P(None, None), whole, P(None, None), P('tp', None), whole, whole, whole, P(None, 'tp'), P('tp'), P('tp', None), whole, whole, whole)
    return jax.shard_map(block_fn, mesh=mesh, in_specs=in_specs, out_specs=band, check_vma=False)
```

```python
import functools
import math
import jax
import jax.numpy as jnp
from jax import lax
from jax.experimental import pallas as pl
from jax.experimental.pallas import tpu as pltpu
from jax.sharding import PartitionSpec as P

WIN = 16
C, U, Q = 1024, 512, 256
LOG2E = 1.4426950408889634
N3, N4, N6, S8, W24, D, LN = 3, 4, 6, 8, 24, 32, 128
F32, BF16 = jnp.float32, jnp.bfloat16
MESH = pl.DeviceIdType.MESH
HALF = 12
EXTRA = 1
AHEAD = 6
NU = HALF + EXTRA
LAG = N4
NEG = -100.0 * LOG2E


def ln_rows(u, gain, bias):
    mean = jnp.mean(u, axis=-1, keepdims=True)
    c = u - mean
    var = jnp.mean(c * c, axis=-1, keepdims=True)
    return c * lax.rsqrt(var + 1e-5) * gain + bias


def kernel(x_ref, wq_in, wp_in, w1_in, w2_in, pack_in, cw1, cb1, cw2, g1, be1, g2, be2,
           out_ref, halo_ref,
           wq, wp, w1, w2, pack, bias, cmask, xb, oT, pring, qTs, kbs, vTs, qss, kis, ub, yb, gb, mb, zb,
           hal_s, hal_r, wz_s, wz_r, wy_s, wy_r, wx_s, wx_r, ws_s, ws_r, pk_s, pk_r, own_s,
           xl, lw, ls, lr, zs, zr):
    dp, z, sp = lax.axis_index("dp"), lax.axis_index("tp"), lax.axis_index("sp")
    half = lax.rem(z, 2)
    end = (z == 0) | (z == N3)
    n = jnp.where(end, NU, HALF)
    k_me = dp * N4 + sp
    ynb, xnb, sib = lax.rem(sp + 2, N4), 1 - dp, sp + 1 - 2 * lax.rem(sp, 2)
    up_sp, dn_sp = lax.rem(sp + 1, N4), lax.rem(sp + N3, N4)
    mats = ((wq_in, wq, LN), (wp_in, wp, D), (w1_in, w1, LN), (w2_in, w2, LN))
    rng = lambda m, k: pl.ds(pl.multiple_of(k * mats[m][2], mats[m][2]), mats[m][2])
    cut = lambda ref, m, k: ref.at[:, rng(m, k)] if m == 0 else ref.at[rng(m, k)]

    def where_is(i):
        uu = jnp.where(i < HALF, i, i - EXTRA)
        hf = jnp.where(i < HALF, half, 1 - half)
        return hf * N3 + uu // N4, lax.rem(uu, N4)

    def cols(jj):
        return (pl.multiple_of(jj * D + S8, S8), pl.multiple_of(jj * D + W24, S8),
                pl.multiple_of(lax.rem(jj * D + D, LN), S8))

    def halo_copies(i):
        b, jj = where_is(i)
        c0, c1, c2 = cols(jj)
        mk = lambda s, d, w: pltpu.make_async_remote_copy(
            src_ref=x_ref.at[b, pl.ds(0, S8), pl.ds(s, w)], dst_ref=halo_ref.at[i, :, pl.ds(d, w)],
            send_sem=hal_s.at[i], recv_sem=hal_r.at[i], device_id=(dp, z, dn_sp), device_id_type=MESH)
        return mk(c0, 0, W24), mk(c2, W24, S8)

    def halo_wait(i):
        return pltpu.make_async_remote_copy(
            src_ref=halo_ref.at[i], dst_ref=halo_ref.at[i], send_sem=hal_s.at[i], recv_sem=hal_r.at[i],
            device_id=(dp, z, dn_sp), device_id_type=MESH)

    def halo_start(i):
        for c in halo_copies(i):
            c.start()

    def piece(m, p, k):
        return cut(mats[m][1].at[p], m, k)

    def own_copy(m):
        return pltpu.make_async_copy(mats[m][0], mats[m][1].at[z], own_s.at[m])

    def remote(src, dst, ssem, rsem, dev):
        return pltpu.make_async_remote_copy(src_ref=src, dst_ref=dst, send_sem=ssem, recv_sem=rsem,
                                            device_id=dev, device_id_type=MESH)

    def shard(i):
        near = jnp.where(z == 0, 1, z - 1)
        next_ = jnp.where(z == 0, 2, jnp.where(z == N3, 1, z + 1))
        return jnp.where(i == 0, near, jnp.where(i == 1, next_, jnp.where(z < 2, N3, 0)))

    k_y = dp * N4 + ynb
    k_x = xnb * N4 + sp
    k_xy = xnb * N4 + ynb
    ks = (k_me, k_y, k_x, k_xy)
    dev_s, dev_y, dev_x = (dp, z, sib), (dp, z, ynb), (xnb, z, sp)
    def z_own(m, q):
        return remote(cut(mats[m][0], m, k_me), piece(m, z, k_me), wz_s.at[m, q - 1], wz_r.at[m, z],
                      (dp, lax.rem(z + q, N4), sp))

    def z_came(m, p):
        ref = piece(m, p, k_me)
        return remote(ref, ref, wz_s.at[m, 0], wz_r.at[m, p], (dp, z, sp))

    def pk_copy(q):
        return remote(pack_in, pack.at[z], pk_s.at[q - 1], pk_r.at[q - 1], (dp, lax.rem(z + q, N4), sp))

    def fwd(m, p, a, sems, b, dev):
        ref = piece(m, p, ks[a])
        return remote(ref, ref, sems[0].at[m, p, b], sems[1].at[m, p, b], dev)

    f_y = lambda m, p, b: fwd(m, p, (0, 2)[b], (wy_s, wy_r), b, dev_y)
    f_x = lambda m, p, b: fwd(m, p, (0, 1)[b], (wx_s, wx_r), b, dev_x)
    f_s = lambda m, p, a: fwd(m, p, a, (ws_s, ws_r), a, dev_s)

    def each_q(f):
        def body(q, c):
            f(q)
            return c
        lax.fori_loop(1, N4, body, 0)

    def via(m, i):
        return ("xyx", "xxx", "xxx", "xyx")[m][i]

    def relay1(m, i):
        p = shard(i)
        z_came(m, p).wait_recv()
        f_x(m, p, 0).start()
        f_y(m, p, 0).start()
        f_s(m, p, 0).start()

    def relay2(m, i):
        p = shard(i)
        f_y(m, p, 0).wait_recv()
        if via(m, i) == "x":
            f_x(m, p, 1).start()
        f_s(m, p, 1).start()

    def relay3(m, i):
        p = shard(i)
        f_x(m, p, 0).wait_recv()
        if via(m, i) == "y":
            f_y(m, p, 1).start()
        f_s(m, p, 2).start()

    def relay4(m, i):
        p = shard(i)
        (f_x if via(m, i) == "x" else f_y)(m, p, 1).wait_recv()
        f_s(m, p, N3).start()

    def arrived(m):
        def f(q):
            p = shard(q - 1)
            for a in range(N4):
                f_s(m, p, a).wait_recv()
        each_q(f)
        own_copy(m).wait()

    def drain_w(m):
        each_q(lambda q: z_own(m, q).wait_send())
        for i in range(N3):
            p = shard(i)
            f_y(m, p, 0).wait_send()
            f_x(m, p, 0).wait_send()
            if via(m, i) == "x":
                f_x(m, p, 1).wait_send()
            if via(m, i) == "y":
                f_y(m, p, 1).wait_send()
            for a in range(N4):
                f_s(m, p, a).wait_send()

    def x_copies(i):
        b, jj = where_is(i)
        c0, c1, c2 = cols(jj)
        sl = lax.rem(i, N4)
        own = lambda c, w: x_ref.at[b, pl.ds(S8, S8), pl.ds(c, w)]
        hal = lambda c, w: halo_ref.at[i, :, pl.ds(c, w)]
        prs = ((own(c0, 16), xb.at[sl, 0, pl.ds(0, S8)]), (hal(0, 16), xb.at[sl, 0, pl.ds(S8, S8)]),
               (own(c1, S8), xb.at[sl, 1, pl.ds(0, S8), pl.ds(0, S8)]), (hal(16, S8), xb.at[sl, 1, pl.ds(S8, S8), pl.ds(0, S8)]),
               (own(c2, S8), xb.at[sl, 1, pl.ds(0, S8), pl.ds(S8, S8)]), (hal(W24, S8), xb.at[sl, 1, pl.ds(S8, S8), pl.ds(S8, S8)]))
        return [pltpu.make_async_copy(s, d, xl.at[sl]) for s, d in prs]

    def x_start(i):
        halo_wait(i).wait_recv()
        for c in x_copies(i):
            c.start()

    def x_wait(i):
        sl = lax.rem(i, N4)
        pltpu.make_async_copy(xb.at[sl], xb.at[sl], xl.at[sl]).wait()

    def z_local(i):
        b, jj = where_is(i)
        c0, c1, c2 = cols(jj)
        sl = lax.rem(i, 2)
        o = lambda c, w: out_ref.at[b, pl.ds(S8, S8), pl.ds(c, w)]
        return [pltpu.make_async_copy(s, d, lw.at[sl]) for s, d in (
            (zb.at[sl, 0, pl.ds(0, S8)], o(c0, 16)),
            (zb.at[sl, 1, pl.ds(0, S8), pl.ds(0, S8)], o(c1, S8)),
            (zb.at[sl, 1, pl.ds(0, S8), pl.ds(S8, S8)], o(c2, S8)))]

    def z_band(i):
        b, jj = where_is(i)
        c0, c1, c2 = cols(jj)
        sl = lax.rem(i, 2)
        o = lambda c, w: out_ref.at[b, pl.ds(0, S8), pl.ds(c, w)]
        return [pltpu.make_async_remote_copy(src_ref=s, dst_ref=d, send_sem=ls.at[sl], recv_sem=lr.at[i],
                                             device_id=(dp, z, up_sp), device_id_type=MESH) for s, d in (
            (zb.at[sl, 0, pl.ds(S8, S8)], o(c0, 16)),
            (zb.at[sl, 1, pl.ds(S8, S8), pl.ds(0, S8)], o(c1, S8)),
            (zb.at[sl, 1, pl.ds(S8, S8), pl.ds(S8, S8)], o(c2, S8)))]

    def z_local_wait(i):
        sl = lax.rem(i, 2)
        ref = zb.at[sl, 0]
        pltpu.make_async_copy(ref, ref, lw.at[sl]).wait()

    def band_waits(i):
        sl = lax.rem(i, 2)
        ref = halo_ref.at[i]
        return pltpu.make_async_remote_copy(src_ref=ref, dst_ref=ref, send_sem=ls.at[sl], recv_sem=lr.at[i],
                                            device_id=(dp, z, up_sp), device_id_type=MESH)

    def z_send(i, h, d):
        b, jj = where_is(i)
        c0, c1, c2 = cols(jj)
        dz = jnp.clip(z + 2 * d - 1, 0, N3)
        r = lambda c, w: out_ref.at[b, pl.ds(S8 * h, S8), pl.ds(c, w)]
        return [pltpu.make_async_remote_copy(src_ref=r(c, w), dst_ref=r(c, w), send_sem=zs.at[d, h, i], recv_sem=zr.at[h, i],
                                             device_id=(dp, dz, sp), device_id_type=MESH) for c, w in ((c0, W24), (c2, S8))]

    def z_send_waits(i, h, d):
        ref = halo_ref.at[0]
        return pltpu.make_async_remote_copy(src_ref=ref, dst_ref=ref, send_sem=zs.at[d, h, i], recv_sem=zr.at[h, i],
                                            device_id=(dp, z, sp), device_id_type=MESH)

    def sends_to(i, d):
        even = lax.rem(i, 2) == 0
        main = i < HALF - EXTRA
        if d == 1:
            ok = ((z <= 1) & even) | ((z == 2) & main)
        else:
            ok = ((z >= 2) & jnp.logical_not(even)) | ((z == 1) & main)
        return ok & (i < HALF)

    def z_send_start(i, h):
        for d in range(2):
            @pl.when(sends_to(i, d))
            def _():
                for c in z_send(i, h, d):
                    c.start()

    dot = lambda a, b: jnp.dot(a, b, preferred_element_type=F32)
    blk = lambda j: slice(j * Q, j * Q + Q)

    def queries(t, g, sl):
        x = lambda: xb[lax.rem(t, N4)].reshape(U, C)
        sq = lambda a: jnp.maximum(jnp.sqrt(jnp.sum(a * a, axis=1)), 1e-12)
        qT = (dot(x(), wq[g, 0]) + pack[g, 1:2, 0:Q]).astype(BF16).T
        qTs[sl] = qT
        qss[sl] = pack[g, S8:16, 0:U] / sq(qT.astype(F32).reshape(S8, D, U))
        kb = dot(x(), wq[g, 1]).astype(BF16)
        kbs[sl] = kb
        kis[sl] = (1.0 / sq(kb.T.astype(F32).reshape(S8, D, U))).T
        vTs[sl] = (dot(x(), wq[g, 2]) + pack[g, 1:2, Q:U]).astype(BF16).T

    def attention(t, g, sl):
        _, jj = where_is(t)
        last = jnp.where(jj == N3, NEG, 0.0)
        par = lax.rem(t, 2)
        hw = [(h, w) for h in range(S8) for w in range(2)]
        rs = {}

        def soft(i):
            h, w = hw[i]
            ts = blk(w)
            parts = [jnp.zeros((D * h, Q), BF16)] if h else []
            parts.append(qTs[sl, D * h:D * h + D, ts])
            if h < 7:
                parts.append(jnp.zeros((224 - D * h, Q), BF16))
            a = dot(kbs[sl, ts, :], jnp.concatenate(parts, axis=0))
            a = a * kis[sl, ts, h:h + 1] * qss[sl, h:h + 1, ts] + bias[g * S8 + h]
            if w:
                a = (a.reshape(WIN, WIN, Q) + (cmask[...] * last)[None]).reshape(Q, Q)
            e = jnp.exp2(a - jnp.max(a, axis=0, keepdims=True))
            rs[i] = 1.0 / jnp.sum(e, axis=0, keepdims=True)
            pring[i % (LAG + 2)] = e.astype(BF16)

        def values(i):
            h, w = hw[i]
            o = dot(vTs[sl, D * h:D * h + D, blk(w)], pring[i % (LAG + 2)])
            oT[par, pl.ds(pl.multiple_of(g * Q + D * h, D), D), blk(w)] = (o * rs[i]).astype(BF16)

        for i in range(WIN + LAG):
            if i < WIN:
                soft(i)
            if i >= LAG:
                values(i - LAG)

    def project(t, g):
        r = pl.ds(pl.multiple_of(g * LN, LN), LN)
        o = oT[lax.rem(t, 2), :, r].T
        for nb in range(N4):
            acc = dot(o[:, blk(0)], wp[0, :, blk(nb)])
            for p in range(1, N4):
                acc += dot(o[:, blk(p)], wp[p, :, blk(nb)])
            ub[:, blk(nb)] = (acc + pack[z, 2:N3, blk(nb)]).astype(BF16)

    def norm1(t, g):
        r = pl.ds(pl.multiple_of(g * LN, LN), LN)
        x = xb[lax.rem(t, N4), g // 2, pl.ds(pl.multiple_of(lax.rem(g, 2) * S8, S8), S8)].reshape(LN, C).astype(F32)
        yb[lax.rem(t, AHEAD), r] = (x + ln_rows(ub[...].astype(F32), g1[...], be1[...])).astype(BF16)

    def up(m, s):
        y = lambda: yb[lax.rem(m, AHEAD)]
        for nb in range(N4):
            h = dot(y(), w1[s, :, blk(nb)]) + pack[s, 0:1, blk(nb)]
            gb[:, blk(nb)] = (0.5 * h * (1.0 + lax.erf(h * math.sqrt(0.5)))).astype(BF16)

    def down(m, s):
        for nb in range(N4):
            mb[lax.rem(m, 2), :, blk(nb)] += dot(gb[...], w2[s, :, blk(nb)])

    def clear(m):
        mb[lax.rem(m, 2)] = jnp.broadcast_to(pack[z, N3:N4], (U, C))

    def norm2(m, g):
        sl = lax.rem(m + 2, 2)
        r = pl.ds(pl.multiple_of(g * LN, LN), LN)
        u = mb[sl, r].astype(BF16).astype(F32)
        zz = yb[lax.rem(m + AHEAD, AHEAD), r].astype(F32) + ln_rows(u, g2[...], be2[...])
        zb[sl, g // 2, pl.ds(pl.multiple_of(lax.rem(g, 2) * S8, S8), S8)] = zz.astype(BF16).reshape(S8, WIN, C)

    def bias_table():
        ql = lax.broadcasted_iota(jnp.int32, (WIN, Q), 1)
        kr = lax.broadcasted_iota(jnp.int32, (WIN, Q), 0)
        cmask[...] = jnp.where((kr < S8) != (lax.rem(ql, WIN) < S8), 1.0, 0.0)
        for part in range(N4):
            row = lax.broadcasted_iota(jnp.int32, (Q, LN), 0) + part * Q

            def coord(d):
                far = jnp.log(1.0 + (8.0 / (WIN - 1)) * jnp.abs(d).astype(F32)) * (LOG2E / 3.0)
                return jnp.concatenate([jnp.where(d < 0, -far, far)] * N4, axis=1)
            hid = coord(row // D - 15) * cw1[0:1] + coord(lax.rem(row, D) - 15) * cw1[1:2] + cb1[...]
            tab = lax.dot_general(cw2[...], jnp.maximum(hid, 0.0), (((1,), (1,)), ((), ())),
                                  precision=lax.Precision.HIGHEST, preferred_element_type=F32)
            mb[0, 0:D, blk(part)] = (WIN * LOG2E) / (1.0 + jnp.exp(-tab))
        row = lax.broadcasted_iota(jnp.int32, (U, Q), 0)
        col = lax.broadcasted_iota(jnp.int32, (U, Q), 1)
        pick = (row // D == col // WIN) & (lax.rem(row, D) == lax.rem(col, WIN))
        gb[:, 0:Q] = jnp.where(pick, 1.0, 0.0).astype(BF16)

    def bias_heads(lo):
        rm = jnp.where(sp == N3, NEG, 0.0)
        ql = lax.broadcasted_iota(jnp.int32, (WIN, Q), 1)
        top = jnp.where(ql >= LN, rm, 0.0)
        bot = jnp.where(ql < LN, rm, 0.0)

        def head(h, carry):
            r = pltpu.roll(jnp.broadcast_to(mb[0, pl.ds(h, 1), :], (WIN, C)), C - 15, 1, stride=1, stride_axis=0)
            terms = []
            for _ in range(N3):
                terms.append(r.astype(BF16))
                r = r - terms[-1].astype(F32)
            terms = jnp.concatenate(terms, axis=0)
            e = []
            for k in range(2):
                p = dot(terms[:, k * U:k * U + U], gb[:, 0:Q])
                e.append(p[0:WIN] + p[WIN:2 * WIN] + p[2 * WIN:])
            e = jnp.concatenate(e, axis=1)
            for ik in range(WIN):
                off = (15 - ik) * WIN
                r = (pltpu.roll(e, U - off, 1) if off else e)[:, 0:Q]
                bias[h, WIN * ik:WIN * ik + WIN, :] = r + (top if ik < S8 else bot)
            return carry
        lax.fori_loop(lo, lo + S8, head, 0)

    def each_g(f):
        def it(g, carry):
            f(g)
            return carry
        lax.fori_loop(0, N4, it, 0)

    halo_start(0)
    for m in range(N4):
        own_copy(m).start()
    pk_own = pltpu.make_async_copy(pack_in, pack.at[z], own_s.at[N4])
    pk_own.start()
    each_q(lambda q: z_own(0, q).start())
    each_q(lambda q: pk_copy(q).start())
    bias_table()
    relay1(0, 0)
    bias_heads(0)
    relay1(0, 1)
    each_q(lambda q: z_own(1, q).start())
    relay2(0, 0)
    x_start(0)
    bias_heads(S8)
    relay3(0, 0)
    relay1(0, 2)
    each_q(lambda q: z_own(2, q).start())
    relay2(0, 1)
    bias_heads(WIN)
    relay3(0, 1)
    halo_start(1)
    relay4(0, 0)
    relay2(0, 2)
    bias_heads(W24)
    relay3(0, 2)
    for i in range(N3):
        relay1(1, i)
    relay4(0, 1)
    for i in range(N3):
        relay2(1, i)
    relay4(0, 2)
    halo_start(2)
    arrived(0)
    each_q(lambda q: pk_copy(q).wait_recv())
    pk_own.wait()
    x_start(1)
    x_wait(0)
    queries(0, 0, 0)

    def service(j):
        @pl.when(j == 1)
        def _():
            each_q(lambda q: z_own(N3, q).start())

        for first, step, f, m in ((1, 1, relay1, 2), (1, 1, relay3, 1), (1, 1, relay4, 1), (5, 1, relay3, 2), (5, 1, relay2, 2),
                                  (7, 1, relay1, N3), (11, 1, relay4, 2), (11, 1, relay2, N3), (14, 1, relay3, N3), (16, 1, relay4, N3)):
            for i in range(N3):
                @pl.when(j == first + i * step)
                def _():
                    f(m, i)

    def pass_on(u, g):
        @pl.when((g == 1) & (u >= 0))
        def _():
            z_local_wait(u)
            z_send_start(u, 1)

        @pl.when((g == N3) & (u >= 0))
        def _():
            band_waits(u).wait_recv()
            z_send_start(u, 0)

    def after(u):
        @pl.when(u >= 0)
        def _():
            for c in z_local(u):
                c.start()
            for c in z_band(u):
                c.start()

    def next_x(t):
        @pl.when(t + 1 < n)
        def _():
            x_wait(t + 1)

        @pl.when(t + 2 < n)
        def _():
            x_start(t + 2)

        @pl.when(t + N3 < n)
        def _():
            halo_start(t + N3)

    def ask(t, g):
        queries(jnp.where(g == N3, jnp.minimum(t + 1, n - 1), t), lax.rem(g + 1, N4), lax.rem(g + 1, 2))

    def first(g):
        service(g)
        ask(0, g)
        attention(0, g, lax.rem(g, 2))
    next_x(0)
    each_g(first)
    arrived(1)

    def upto(t):
        return jnp.where(t < AHEAD - 1, 0, jnp.where(t < n, t - AHEAD + N3, n))

    def tick(t, carry):
        lo, hi = upto(t - 1), upto(t)

        @pl.when(t == AHEAD - 1)
        def _():
            arrived(2)
            arrived(N3)

        @pl.when(t == n)
        def _():
            def finish(g):
                project(n - 1, g)
                norm1(n - 1, g)
            each_g(finish)

        def mlp(m, c):
            @pl.when(m >= N3)
            def _():
                band_waits(m - N3).wait_send()
            clear(m)

            def it(g):
                pass_on(jnp.where(m > lo, m - 2, -1), g)
                up(m, g)
                norm2(m - 1, g)
                down(m, g)
            each_g(it)
            after(m - 1)
            return c
        lax.fori_loop(lo, hi, mlp, 0)

        @pl.when(t < n)
        def _():
            next_x(t)

            def it(g):
                service(N4 * t + g)
                pass_on(hi - 2, g)
                project(t - 1, g)
                ask(t, g)
                norm1(t - 1, g)
                attention(t, g, lax.rem(g, 2))
            each_g(it)
        return carry
    lax.fori_loop(1, n + 1, tick, 0)
    band_waits(n - N3).wait_send()

    def last(g):
        pass_on(n - 2, g)
        norm2(n - 1, g)
    each_g(last)
    after(n - 1)
    band_waits(n - 2).wait_send()
    z_local_wait(n - 1)
    z_send_start(n - 1, 1)
    band_waits(n - 1).wait_send()
    band_waits(n - 1).wait_recv()
    z_send_start(n - 1, 0)

    def drain(i, carry):
        halo_wait(i).wait_send()
        for h in range(2):
            for d in range(2):
                @pl.when(sends_to(i, d))
                def _():
                    z_send_waits(i, h, d).wait_send()
        return carry
    lax.fori_loop(0, n, drain, 0)
    for m in range(N4):
        drain_w(m)
    each_q(lambda q: pk_copy(q).wait_send())

    def arrive(i, carry):
        for h in range(2):
            z_send_waits(i, h, 0).wait_recv()
        return carry
    lax.fori_loop(0, jnp.where(end, HALF - EXTRA, HALF), arrive, 0)


def block(*args):
    hbm = pl.BlockSpec(memory_space=pl.ANY)
    vm = pl.BlockSpec(memory_space=pltpu.VMEM)
    dma, V = pltpu.SemaphoreType.DMA, pltpu.VMEM
    out, _ = pl.pallas_call(
        kernel, name="swin",
        out_shape=(jax.ShapeDtypeStruct(args[0].shape, BF16), jax.ShapeDtypeStruct((NU, S8, D, C), BF16)),
        in_specs=[hbm] * N6 + [vm] * 7, out_specs=(hbm, hbm),
        scratch_shapes=[
            V((N4, N3, C, Q), BF16), V((N4, Q, C), BF16), V((N4, C, C), BF16), V((N4, C, C), BF16), V((N4, WIN, C), F32),
            V((D, Q, Q), F32), V((WIN, Q), F32), V((N4, 2, WIN, WIN, C), BF16), V((2, C, U), BF16), V((LAG + 2, Q, Q), BF16),
            V((2, Q, U), BF16), V((2, U, Q), BF16), V((2, Q, U), BF16), V((2, S8, U), F32), V((2, U, S8), F32),
            V((LN, C), BF16), V((AHEAD, U, C), BF16), V((U, C), BF16), V((2, U, C), F32), V((2, 2, WIN, WIN, C), BF16),
            dma((NU,)), dma((NU,)), dma((N4, N3)), dma((N4, N4)), dma((N4, N4, 2)), dma((N4, N4, 2)),
            dma((N4, N4, 2)), dma((N4, N4, 2)), dma((N4, N4, N4)), dma((N4, N4, N4)), dma((N3,)), dma((N3,)), dma((5,)),
            dma((N4,)), dma((2,)), dma((2,)), dma((NU,)), dma((2, 2, NU)), dma((2, HALF))],
        compiler_params=pltpu.CompilerParams(has_side_effects=True, vmem_limit_bytes=67_000_000),
    )(*args)
    return out


def solution(mesh):
    def block_fn(x, w_qkv, q_bias, v_bias, logit_scale, cpb_w1, cpb_b1, cpb_w2, w_proj, b_proj, g1, be1, w_fc1, b_fc1, w_fc2, b_fc2, g2, be2):
        hs = jnp.exp(jnp.minimum(logit_scale, math.log(100.0))) * LOG2E
        r = lax.broadcasted_iota(jnp.int32, (WIN, C), 0)
        qv = jnp.pad(q_bias, (0, C - Q)).astype(F32) + jnp.pad(v_bias, (Q, U)).astype(F32)
        pack = jnp.where(r == 0, b_fc1.astype(F32)[None], jnp.where(r == 1, qv[None], jnp.where(
            r == 2, b_proj.astype(F32)[None], jnp.where(r == N3, b_fc2.astype(F32)[None], jnp.pad(hs, (S8, 0))[:, None]))))
        row = lambda a: a.reshape(1, -1)
        return block(x, w_qkv.transpose(1, 0, 2), w_proj, w_fc1, w_fc2, pack, cpb_w1, row(cpb_b1), cpb_w2.T,
                     row(g1), row(be1), row(g2), row(be2))

    band = P('dp', 'sp', None, None)
    whole = P(None)
    in_specs = (band, P(None, None, 'tp'), P('tp'), P('tp'), P('tp'), P(None, None), whole, P(None, None), P('tp', None), whole, whole, whole, P(None, 'tp'), P('tp'), P('tp', None), whole, whole, whole)
    return jax.shard_map(block_fn, mesh=mesh, in_specs=in_specs, out_specs=band, check_vma=False)
```

```python
import functools
import math
import jax
import jax.numpy as jnp
from jax import lax
from jax.experimental import pallas as pl
from jax.experimental.pallas import tpu as pltpu
from jax.sharding import PartitionSpec as P

WIN = 16
C, U, Q = 1024, 512, 256
LOG2E = 1.4426950408889634
N3, N4, N6, S8, W24, D, LN = 3, 4, 6, 8, 24, 32, 128
F32, BF16 = jnp.float32, jnp.bfloat16
MESH = pl.DeviceIdType.MESH
HALF = 12
EXTRA = 1
AHEAD = 6
NU = HALF + EXTRA
LAG = N4
NEG = -100.0 * LOG2E


def ln_rows(u, gain, bias):
    mean = jnp.mean(u, axis=-1, keepdims=True)
    c = u - mean
    var = jnp.mean(c * c, axis=-1, keepdims=True)
    return c * lax.rsqrt(var + 1e-5) * gain + bias


def kernel(x_ref, wq_in, wp_in, w1_in, w2_in, pack_in, cw1, cb1, cw2, g1, be1, g2, be2,
           out_ref, halo_ref,
           wq, wp, w1, w2, pack, bias, cmask, xb, oT, pring, qTs, kbs, vTs, qss, kis, ub, yb, gb, mb, zb,
           hal_s, hal_r, wz_s, wz_r, wy_s, wy_r, wx_s, wx_r, ws_s, ws_r, pk_s, pk_r, own_s,
           xl, lw, ls, lr, zs, zr):
    dp, z, sp = lax.axis_index("dp"), lax.axis_index("tp"), lax.axis_index("sp")
    half = lax.rem(z, 2)
    end = (z == 0) | (z == N3)
    n = jnp.where(end, NU, HALF)
    k_me = dp * N4 + sp
    ynb, xnb, sib = lax.rem(sp + 2, N4), 1 - dp, sp + 1 - 2 * lax.rem(sp, 2)
    up_sp, dn_sp = lax.rem(sp + 1, N4), lax.rem(sp + N3, N4)
    mats = ((wq_in, wq, LN), (wp_in, wp, D), (w1_in, w1, LN), (w2_in, w2, LN))
    rng = lambda m, k: pl.ds(pl.multiple_of(k * mats[m][2], mats[m][2]), mats[m][2])
    cut = lambda ref, m, k: ref.at[:, rng(m, k)] if m == 0 else ref.at[rng(m, k)]

    def where_is(i):
        uu = jnp.where(i < HALF, i, i - EXTRA)
        hf = jnp.where(i < HALF, half, 1 - half)
        return hf * N3 + uu // N4, lax.rem(uu, N4)

    def cols(jj):
        return (pl.multiple_of(jj * D + S8, S8), pl.multiple_of(jj * D + W24, S8),
                pl.multiple_of(lax.rem(jj * D + D, LN), S8))

    def halo_copies(i):
        b, jj = where_is(i)
        c0, c1, c2 = cols(jj)
        mk = lambda s, d, w: pltpu.make_async_remote_copy(
            src_ref=x_ref.at[b, pl.ds(0, S8), pl.ds(s, w)], dst_ref=halo_ref.at[i, :, pl.ds(d, w)],
            send_sem=hal_s.at[i], recv_sem=hal_r.at[i], device_id=(dp, z, dn_sp), device_id_type=MESH)
        return mk(c0, 0, W24), mk(c2, W24, S8)

    def halo_wait(i):
        return pltpu.make_async_remote_copy(
            src_ref=halo_ref.at[i], dst_ref=halo_ref.at[i], send_sem=hal_s.at[i], recv_sem=hal_r.at[i],
            device_id=(dp, z, dn_sp), device_id_type=MESH)

    def halo_start(i):
        for c in halo_copies(i):
            c.start()

    def piece(m, p, k):
        return cut(mats[m][1].at[p], m, k)

    def own_copy(m):
        return pltpu.make_async_copy(mats[m][0], mats[m][1].at[z], own_s.at[m])

    def remote(src, dst, ssem, rsem, dev):
        return pltpu.make_async_remote_copy(src_ref=src, dst_ref=dst, send_sem=ssem, recv_sem=rsem,
                                            device_id=dev, device_id_type=MESH)

    def shard(i):
        near = jnp.where(z == 0, 1, z - 1)
        next_ = jnp.where(z == 0, 2, jnp.where(z == N3, 1, z + 1))
        return jnp.where(i == 0, near, jnp.where(i == 1, next_, jnp.where(z < 2, N3, 0)))

    k_y = dp * N4 + ynb
    k_x = xnb * N4 + sp
    k_xy = xnb * N4 + ynb
    ks = (k_me, k_y, k_x, k_xy)
    dev_s, dev_y, dev_x = (dp, z, sib), (dp, z, ynb), (xnb, z, sp)
    def z_own(m, q):
        return remote(cut(mats[m][0], m, k_me), piece(m, z, k_me), wz_s.at[m, q - 1], wz_r.at[m, z],
                      (dp, lax.rem(z + q, N4), sp))

    def z_came(m, p):
        ref = piece(m, p, k_me)
        return remote(ref, ref, wz_s.at[m, 0], wz_r.at[m, p], (dp, z, sp))

    def pk_copy(q):
        return remote(pack_in, pack.at[z], pk_s.at[q - 1], pk_r.at[q - 1], (dp, lax.rem(z + q, N4), sp))

    def fwd(m, p, a, sems, b, dev):
        ref = piece(m, p, ks[a])
        return remote(ref, ref, sems[0].at[m, p, b], sems[1].at[m, p, b], dev)

    f_y = lambda m, p, b: fwd(m, p, (0, 2)[b], (wy_s, wy_r), b, dev_y)
    f_x = lambda m, p, b: fwd(m, p, (0, 1)[b], (wx_s, wx_r), b, dev_x)
    f_s = lambda m, p, a: fwd(m, p, a, (ws_s, ws_r), a, dev_s)

    def each_q(f):
        def body(q, c):
            f(q)
            return c
        lax.fori_loop(1, N4, body, 0)

    def via(m, i):
        return ("xyx", "xxx", "xxx", "xyx")[m][i]

    def relay1(m, i):
        p = shard(i)
        z_came(m, p).wait_recv()
        f_x(m, p, 0).start()
        f_y(m, p, 0).start()
        f_s(m, p, 0).start()

    def relay2(m, i):
        p = shard(i)
        f_y(m, p, 0).wait_recv()
        if via(m, i) == "x":
            f_x(m, p, 1).start()
        f_s(m, p, 1).start()

    def relay3(m, i):
        p = shard(i)
        f_x(m, p, 0).wait_recv()
        if via(m, i) == "y":
            f_y(m, p, 1).start()
        f_s(m, p, 2).start()

    def relay4(m, i):
        p = shard(i)
        (f_x if via(m, i) == "x" else f_y)(m, p, 1).wait_recv()
        f_s(m, p, N3).start()

    def arrived(m):
        def f(q):
            p = shard(q - 1)
            for a in range(N4):
                f_s(m, p, a).wait_recv()
        each_q(f)
        own_copy(m).wait()

    def drain_w(m):
        each_q(lambda q: z_own(m, q).wait_send())
        for i in range(N3):
            p = shard(i)
            f_y(m, p, 0).wait_send()
            f_x(m, p, 0).wait_send()
            if via(m, i) == "x":
                f_x(m, p, 1).wait_send()
            if via(m, i) == "y":
                f_y(m, p, 1).wait_send()
            for a in range(N4):
                f_s(m, p, a).wait_send()

    def x_copies(i):
        b, jj = where_is(i)
        c0, c1, c2 = cols(jj)
        sl = lax.rem(i, N4)
        own = lambda c, w: x_ref.at[b, pl.ds(S8, S8), pl.ds(c, w)]
        hal = lambda c, w: halo_ref.at[i, :, pl.ds(c, w)]
        prs = ((own(c0, 16), xb.at[sl, 0, pl.ds(0, S8)]), (hal(0, 16), xb.at[sl, 0, pl.ds(S8, S8)]),
               (own(c1, S8), xb.at[sl, 1, pl.ds(0, S8), pl.ds(0, S8)]), (hal(16, S8), xb.at[sl, 1, pl.ds(S8, S8), pl.ds(0, S8)]),
               (own(c2, S8), xb.at[sl, 1, pl.ds(0, S8), pl.ds(S8, S8)]), (hal(W24, S8), xb.at[sl, 1, pl.ds(S8, S8), pl.ds(S8, S8)]))
        return [pltpu.make_async_copy(s, d, xl.at[sl]) for s, d in prs]

    def x_start(i):
        halo_wait(i).wait_recv()
        for c in x_copies(i):
            c.start()

    def x_wait(i):
        sl = lax.rem(i, N4)
        pltpu.make_async_copy(xb.at[sl], xb.at[sl], xl.at[sl]).wait()

    def z_local(i):
        b, jj = where_is(i)
        c0, c1, c2 = cols(jj)
        sl = lax.rem(i, 2)
        o = lambda c, w: out_ref.at[b, pl.ds(S8, S8), pl.ds(c, w)]
        return [pltpu.make_async_copy(s, d, lw.at[sl]) for s, d in (
            (zb.at[sl, 0, pl.ds(0, S8)], o(c0, 16)),
            (zb.at[sl, 1, pl.ds(0, S8), pl.ds(0, S8)], o(c1, S8)),
            (zb.at[sl, 1, pl.ds(0, S8), pl.ds(S8, S8)], o(c2, S8)))]

    def z_band(i):
        b, jj = where_is(i)
        c0, c1, c2 = cols(jj)
        sl = lax.rem(i, 2)
        o = lambda c, w: out_ref.at[b, pl.ds(0, S8), pl.ds(c, w)]
        return [pltpu.make_async_remote_copy(src_ref=s, dst_ref=d, send_sem=ls.at[sl], recv_sem=lr.at[i],
                                             device_id=(dp, z, up_sp), device_id_type=MESH) for s, d in (
            (zb.at[sl, 0, pl.ds(S8, S8)], o(c0, 16)),
            (zb.at[sl, 1, pl.ds(S8, S8), pl.ds(0, S8)], o(c1, S8)),
            (zb.at[sl, 1, pl.ds(S8, S8), pl.ds(S8, S8)], o(c2, S8)))]

    def z_local_wait(i):
        sl = lax.rem(i, 2)
        ref = zb.at[sl, 0]
        pltpu.make_async_copy(ref, ref, lw.at[sl]).wait()

    def band_waits(i):
        sl = lax.rem(i, 2)
        ref = halo_ref.at[i]
        return pltpu.make_async_remote_copy(src_ref=ref, dst_ref=ref, send_sem=ls.at[sl], recv_sem=lr.at[i],
                                            device_id=(dp, z, up_sp), device_id_type=MESH)

    def z_send(i, h, d):
        b, jj = where_is(i)
        c0, c1, c2 = cols(jj)
        dz = jnp.clip(z + 2 * d - 1, 0, N3)
        r = lambda c, w: out_ref.at[b, pl.ds(S8 * h, S8), pl.ds(c, w)]
        return [pltpu.make_async_remote_copy(src_ref=r(c, w), dst_ref=r(c, w), send_sem=zs.at[d, h, i], recv_sem=zr.at[h, i],
                                             device_id=(dp, dz, sp), device_id_type=MESH) for c, w in ((c0, W24), (c2, S8))]

    def z_send_waits(i, h, d):
        ref = halo_ref.at[0]
        return pltpu.make_async_remote_copy(src_ref=ref, dst_ref=ref, send_sem=zs.at[d, h, i], recv_sem=zr.at[h, i],
                                            device_id=(dp, z, sp), device_id_type=MESH)

    def sends_to(i, d):
        even = lax.rem(i, 2) == 0
        main = i < HALF - EXTRA
        if d == 1:
            ok = ((z <= 1) & even) | ((z == 2) & main)
        else:
            ok = ((z >= 2) & jnp.logical_not(even)) | ((z == 1) & main)
        return ok & (i < HALF)

    def z_send_start(i, h):
        for d in range(2):
            @pl.when(sends_to(i, d))
            def _():
                for c in z_send(i, h, d):
                    c.start()

    dot = lambda a, b: jnp.dot(a, b, preferred_element_type=F32)
    blk = lambda j: slice(j * Q, j * Q + Q)

    def queries(t, g, sl):
        x = lambda: xb[lax.rem(t, N4)].reshape(U, C)
        sq = lambda a: jnp.maximum(jnp.sqrt(jnp.sum(a * a, axis=1)), 1e-12)
        qT = (dot(x(), wq[g, 0]) + pack[g, 1:2, 0:Q]).astype(BF16).T
        qTs[sl] = qT
        qss[sl] = pack[g, S8:16, 0:U] / sq(qT.astype(F32).reshape(S8, D, U))
        kb = dot(x(), wq[g, 1]).astype(BF16)
        kbs[sl] = kb
        kis[sl] = (1.0 / sq(kb.T.astype(F32).reshape(S8, D, U))).T
        vTs[sl] = (dot(x(), wq[g, 2]) + pack[g, 1:2, Q:U]).astype(BF16).T

    def attention(t, g, sl):
        _, jj = where_is(t)
        last = jnp.where(jj == N3, NEG, 0.0)
        par = lax.rem(t, 2)
        hw = [(h, w) for h in range(S8) for w in range(2)]
        rs = {}

        def soft(i):
            h, w = hw[i]
            ts = blk(w)
            parts = [jnp.zeros((D * h, Q), BF16)] if h else []
            parts.append(qTs[sl, D * h:D * h + D, ts])
            if h < 7:
                parts.append(jnp.zeros((224 - D * h, Q), BF16))
            a = dot(kbs[sl, ts, :], jnp.concatenate(parts, axis=0))
            a = a * kis[sl, ts, h:h + 1] * qss[sl, h:h + 1, ts] + bias[g * S8 + h]
            if w:
                a = (a.reshape(WIN, WIN, Q) + (cmask[...] * last)[None]).reshape(Q, Q)
            e = jnp.exp2(a - jnp.max(a, axis=0, keepdims=True))
            rs[i] = 1.0 / jnp.sum(e, axis=0, keepdims=True)
            pring[i % (LAG + 2)] = e.astype(BF16)

        def values(i):
            h, w = hw[i]
            o = dot(vTs[sl, D * h:D * h + D, blk(w)], pring[i % (LAG + 2)])
            oT[par, pl.ds(pl.multiple_of(g * Q + D * h, D), D), blk(w)] = (o * rs[i]).astype(BF16)

        for i in range(WIN + LAG):
            if i < WIN:
                soft(i)
            if i >= LAG:
                values(i - LAG)

    def project(t, g):
        r = pl.ds(pl.multiple_of(g * LN, LN), LN)
        o = oT[lax.rem(t, 2), :, r].T
        for nb in range(N4):
            acc = dot(o[:, blk(0)], wp[0, :, blk(nb)])
            for p in range(1, N4):
                acc += dot(o[:, blk(p)], wp[p, :, blk(nb)])
            ub[:, blk(nb)] = (acc + pack[z, 2:N3, blk(nb)]).astype(BF16)

    def norm1(t, g):
        r = pl.ds(pl.multiple_of(g * LN, LN), LN)
        x = xb[lax.rem(t, N4), g // 2, pl.ds(pl.multiple_of(lax.rem(g, 2) * S8, S8), S8)].reshape(LN, C).astype(F32)
        yb[lax.rem(t, AHEAD), r] = (x + ln_rows(ub[...].astype(F32), g1[...], be1[...])).astype(BF16)

    def up(m, s):
        y = lambda: yb[lax.rem(m, AHEAD)]
        for nb in range(N4):
            h = dot(y(), w1[s, :, blk(nb)]) + pack[s, 0:1, blk(nb)]
            gb[:, blk(nb)] = (0.5 * h * (1.0 + lax.erf(h * math.sqrt(0.5)))).astype(BF16)

    def down(m, s):
        for nb in range(N4):
            mb[lax.rem(m, 2), :, blk(nb)] += dot(gb[...], w2[s, :, blk(nb)])

    def clear(m):
        mb[lax.rem(m, 2)] = jnp.broadcast_to(pack[z, N3:N4], (U, C))

    def norm2(m, g):
        sl = lax.rem(m + 2, 2)
        r = pl.ds(pl.multiple_of(g * LN, LN), LN)
        u = mb[sl, r].astype(BF16).astype(F32)
        mb[sl, r] = jnp.broadcast_to(pack[z, N3:N4], (LN, C))
        zz = yb[lax.rem(m + AHEAD, AHEAD), r].astype(F32) + ln_rows(u, g2[...], be2[...])
        zb[sl, g // 2, pl.ds(pl.multiple_of(lax.rem(g, 2) * S8, S8), S8)] = zz.astype(BF16).reshape(S8, WIN, C)

    def bias_table():
        ql = lax.broadcasted_iota(jnp.int32, (WIN, Q), 1)
        kr = lax.broadcasted_iota(jnp.int32, (WIN, Q), 0)
        cmask[...] = jnp.where((kr < S8) != (lax.rem(ql, WIN) < S8), 1.0, 0.0)
        for part in range(N4):
            row = lax.broadcasted_iota(jnp.int32, (Q, LN), 0) + part * Q

            def coord(d):
                far = jnp.log(1.0 + (8.0 / (WIN - 1)) * jnp.abs(d).astype(F32)) * (LOG2E / 3.0)
                return jnp.concatenate([jnp.where(d < 0, -far, far)] * N4, axis=1)
            hid = coord(row // D - 15) * cw1[0:1] + coord(lax.rem(row, D) - 15) * cw1[1:2] + cb1[...]
            tab = lax.dot_general(cw2[...], jnp.maximum(hid, 0.0), (((1,), (1,)), ((), ())),
                                  precision=lax.Precision.HIGHEST, preferred_element_type=F32)
            mb[0, 0:D, blk(part)] = (WIN * LOG2E) / (1.0 + jnp.exp(-tab))
        row = lax.broadcasted_iota(jnp.int32, (U, Q), 0)
        col = lax.broadcasted_iota(jnp.int32, (U, Q), 1)
        pick = (row // D == col // WIN) & (lax.rem(row, D) == lax.rem(col, WIN))
        gb[:, 0:Q] = jnp.where(pick, 1.0, 0.0).astype(BF16)

    def bias_heads(lo):
        rm = jnp.where(sp == N3, NEG, 0.0)
        ql = lax.broadcasted_iota(jnp.int32, (WIN, Q), 1)
        top = jnp.where(ql >= LN, rm, 0.0)
        bot = jnp.where(ql < LN, rm, 0.0)

        def head(h, carry):
            r = pltpu.roll(jnp.broadcast_to(mb[0, pl.ds(h, 1), :], (WIN, C)), C - 15, 1, stride=1, stride_axis=0)
            terms = []
            for _ in range(N3):
                terms.append(r.astype(BF16))
                r = r - terms[-1].astype(F32)
            terms = jnp.concatenate(terms, axis=0)
            e = []
            for k in range(2):
                p = dot(terms[:, k * U:k * U + U], gb[:, 0:Q])
                e.append(p[0:WIN] + p[WIN:2 * WIN] + p[2 * WIN:])
            e = jnp.concatenate(e, axis=1)
            for ik in range(WIN):
                off = (15 - ik) * WIN
                r = (pltpu.roll(e, U - off, 1) if off else e)[:, 0:Q]
                bias[h, WIN * ik:WIN * ik + WIN, :] = r + (top if ik < S8 else bot)
            return carry
        lax.fori_loop(lo, lo + S8, head, 0)

    def each_g(f):
        def it(g, carry):
            f(g)
            return carry
        lax.fori_loop(0, N4, it, 0)

    halo_start(0)
    for m in range(N4):
        own_copy(m).start()
    pk_own = pltpu.make_async_copy(pack_in, pack.at[z], own_s.at[N4])
    pk_own.start()
    each_q(lambda q: z_own(0, q).start())
    each_q(lambda q: pk_copy(q).start())
    bias_table()
    relay1(0, 0)
    bias_heads(0)
    relay1(0, 1)
    each_q(lambda q: z_own(1, q).start())
    relay2(0, 0)
    x_start(0)
    bias_heads(S8)
    relay3(0, 0)
    relay1(0, 2)
    each_q(lambda q: z_own(2, q).start())
    relay2(0, 1)
    bias_heads(WIN)
    relay3(0, 1)
    halo_start(1)
    relay4(0, 0)
    relay2(0, 2)
    bias_heads(W24)
    relay3(0, 2)
    for i in range(N3):
        relay1(1, i)
    relay4(0, 1)
    for i in range(N3):
        relay2(1, i)
    relay4(0, 2)
    halo_start(2)
    arrived(0)
    each_q(lambda q: pk_copy(q).wait_recv())
    pk_own.wait()
    x_start(1)
    x_wait(0)
    queries(0, 0, 0)
    clear(0)
    clear(1)

    def service(j):
        @pl.when(j == 1)
        def _():
            each_q(lambda q: z_own(N3, q).start())

        for first, step, f, m in ((1, 1, relay1, 2), (1, 1, relay3, 1), (1, 1, relay4, 1), (5, 1, relay3, 2), (5, 1, relay2, 2),
                                  (7, 1, relay1, N3), (11, 1, relay4, 2), (11, 1, relay2, N3), (14, 1, relay3, N3), (16, 1, relay4, N3)):
            for i in range(N3):
                @pl.when(j == first + i * step)
                def _():
                    f(m, i)

    def pass_on(u, g):
        @pl.when((g == 1) & (u >= 0))
        def _():
            z_local_wait(u)
            z_send_start(u, 1)

        @pl.when((g == N3) & (u >= 0))
        def _():
            band_waits(u).wait_recv()
            z_send_start(u, 0)

    def after(u):
        @pl.when(u >= 0)
        def _():
            for c in z_local(u):
                c.start()
            for c in z_band(u):
                c.start()

    def next_x(t):
        @pl.when(t + 1 < n)
        def _():
            x_wait(t + 1)

        @pl.when(t + 2 < n)
        def _():
            x_start(t + 2)

        @pl.when(t + N3 < n)
        def _():
            halo_start(t + N3)

    def ask(t, g):
        queries(jnp.where(g == N3, jnp.minimum(t + 1, n - 1), t), lax.rem(g + 1, N4), lax.rem(g + 1, 2))

    def first(g):
        service(g)
        ask(0, g)
        attention(0, g, lax.rem(g, 2))
    next_x(0)
    each_g(first)
    arrived(1)

    def upto(t):
        return jnp.where(t < AHEAD - 1, 0, jnp.where(t < n, t - AHEAD + N3, n))

    def tick(t, carry):
        lo, hi = upto(t - 1), upto(t)

        @pl.when(t == AHEAD - 1)
        def _():
            arrived(2)
            arrived(N3)

        @pl.when(t == n)
        def _():
            def finish(g):
                project(n - 1, g)
                norm1(n - 1, g)
            each_g(finish)

        def mlp(m, c):
            @pl.when(m >= N3)
            def _():
                band_waits(m - N3).wait_send()

            def it(g):
                pass_on(jnp.where(m > lo, m - 2, -1), g)
                up(m, g)
                norm2(m - 1, g)
                down(m, g)
            each_g(it)
            after(m - 1)
            return c
        lax.fori_loop(lo, hi, mlp, 0)

        @pl.when(t < n)
        def _():
            next_x(t)

            def it(g):
                service(N4 * t + g)
                pass_on(hi - 2, g)
                project(t - 1, g)
                ask(t, g)
                norm1(t - 1, g)
                attention(t, g, lax.rem(g, 2))
            each_g(it)
        return carry
    lax.fori_loop(1, n + 1, tick, 0)
    band_waits(n - N3).wait_send()

    def last(g):
        pass_on(n - 2, g)
        norm2(n - 1, g)
    each_g(last)
    after(n - 1)
    band_waits(n - 2).wait_send()
    z_local_wait(n - 1)
    z_send_start(n - 1, 1)
    band_waits(n - 1).wait_send()
    band_waits(n - 1).wait_recv()
    z_send_start(n - 1, 0)

    def drain(i, carry):
        halo_wait(i).wait_send()
        for h in range(2):
            for d in range(2):
                @pl.when(sends_to(i, d))
                def _():
                    z_send_waits(i, h, d).wait_send()
        return carry
    lax.fori_loop(0, n, drain, 0)
    for m in range(N4):
        drain_w(m)
    each_q(lambda q: pk_copy(q).wait_send())

    def arrive(i, carry):
        for h in range(2):
            z_send_waits(i, h, 0).wait_recv()
        return carry
    lax.fori_loop(0, jnp.where(end, HALF - EXTRA, HALF), arrive, 0)


def block(*args):
    hbm = pl.BlockSpec(memory_space=pl.ANY)
    vm = pl.BlockSpec(memory_space=pltpu.VMEM)
    dma, V = pltpu.SemaphoreType.DMA, pltpu.VMEM
    out, _ = pl.pallas_call(
        kernel, name="swin",
        out_shape=(jax.ShapeDtypeStruct(args[0].shape, BF16), jax.ShapeDtypeStruct((NU, S8, D, C), BF16)),
        in_specs=[hbm] * N6 + [vm] * 7, out_specs=(hbm, hbm),
        scratch_shapes=[
            V((N4, N3, C, Q), BF16), V((N4, Q, C), BF16), V((N4, C, C), BF16), V((N4, C, C), BF16), V((N4, WIN, C), F32),
            V((D, Q, Q), F32), V((WIN, Q), F32), V((N4, 2, WIN, WIN, C), BF16), V((2, C, U), BF16), V((LAG + 2, Q, Q), BF16),
            V((2, Q, U), BF16), V((2, U, Q), BF16), V((2, Q, U), BF16), V((2, S8, U), F32), V((2, U, S8), F32),
            V((LN, C), BF16), V((AHEAD, U, C), BF16), V((U, C), BF16), V((2, U, C), F32), V((2, 2, WIN, WIN, C), BF16),
            dma((NU,)), dma((NU,)), dma((N4, N3)), dma((N4, N4)), dma((N4, N4, 2)), dma((N4, N4, 2)),
            dma((N4, N4, 2)), dma((N4, N4, 2)), dma((N4, N4, N4)), dma((N4, N4, N4)), dma((N3,)), dma((N3,)), dma((5,)),
            dma((N4,)), dma((2,)), dma((2,)), dma((NU,)), dma((2, 2, NU)), dma((2, HALF))],
        compiler_params=pltpu.CompilerParams(has_side_effects=True, vmem_limit_bytes=67_000_000),
    )(*args)
    return out


def solution(mesh):
    def block_fn(x, w_qkv, q_bias, v_bias, logit_scale, cpb_w1, cpb_b1, cpb_w2, w_proj, b_proj, g1, be1, w_fc1, b_fc1, w_fc2, b_fc2, g2, be2):
        hs = jnp.exp(jnp.minimum(logit_scale, math.log(100.0))) * LOG2E
        r = lax.broadcasted_iota(jnp.int32, (WIN, C), 0)
        qv = jnp.pad(q_bias, (0, C - Q)).astype(F32) + jnp.pad(v_bias, (Q, U)).astype(F32)
        pack = jnp.where(r == 0, b_fc1.astype(F32)[None], jnp.where(r == 1, qv[None], jnp.where(
            r == 2, b_proj.astype(F32)[None], jnp.where(r == N3, b_fc2.astype(F32)[None], jnp.pad(hs, (S8, 0))[:, None]))))
        row = lambda a: a.reshape(1, -1)
        return block(x, w_qkv.transpose(1, 0, 2), w_proj, w_fc1, w_fc2, pack, cpb_w1, row(cpb_b1), cpb_w2.T,
                     row(g1), row(be1), row(g2), row(be2))

    band = P('dp', 'sp', None, None)
    whole = P(None)
    in_specs = (band, P(None, None, 'tp'), P('tp'), P('tp'), P('tp'), P(None, None), whole, P(None, None), P('tp', None), whole, whole, whole, P(None, 'tp'), P('tp'), P('tp', None), whole, whole, whole)
    return jax.shard_map(block_fn, mesh=mesh, in_specs=in_specs, out_specs=band, check_vma=False)
```
